32 devices in a mesh: dp: 2 (over z, core), ep: 16 (over x, y).
Axes of the slice: x: 4, y: 4, z: 1, core: 2. Of those that a mesh axis runs over, the one named last changes fastest.
The devices are a block of a 4x4x8 slice.
Arguments:
- x: bfloat16 [2, 16, 256, 2560], P('dp', 'ep'), parts along dimension 0
- expert: int32 [2, 16, 256, 6], P('dp', 'ep'), parts along dimension 0
- slot: int32 [2, 16, 256, 6], P('dp', 'ep'), parts along dimension 0
- gate: float32 [2, 16, 256, 6], P('dp', 'ep'), parts along dimension 0
- w_gate: bfloat16 [80, 2560, 1536], P('ep')
- w_up: bfloat16 [80, 2560, 1536], P('ep')
- w_down: bfloat16 [80, 1536, 2560], P('ep')
- s_gate: bfloat16 [2560, 3072], replicated
- s_up: bfloat16 [2560, 3072], replicated
- s_down: bfloat16 [3072, 2560], replicated
Outputs:
- y: bfloat16 [2, 16, 256, 2560], P('dp', 'ep'), parts along dimension 0
There are 2 independent parts. The reference program is written for one: setup_inputs(seed, part) draws one part's arguments, and reference() takes and returns one part's arrays. A program takes and returns all parts, laid end to end along the dimension named above; an argument that names none is the same for every part.
All inputs are finite; a program needn't handle non-finite values.
Results may differ from the reference program's by a relative error of at most 0.009.
Values are sent between devices in bfloat16 or wider.
A program may use at most 768 MiB of HBM per device.

```python
import jax
import jax.numpy as jnp

MEMBERS = 16
TOKENS = 256
D = 2560
FF = 1536
TOP = 6
EXPERTS = 80
SHARED_FF = 3072
SLOTS = 5 * TOKENS * TOP // (4 * EXPERTS)


def setup_inputs(seed: int = 0, part: int = 0) -> dict:
    own, k1, k2, k3, k4, k5, k6 = jax.random.split(jax.random.key(seed), 7)
    kx, ke, kl, kg = jax.random.split(jax.random.fold_in(own, part), 4)
    devices = (1, MEMBERS)
    place = jax.random.permutation(kl, jnp.arange(EXPERTS, dtype=jnp.uint32))
    slow = ((EXPERTS + (9 * place) % EXPERTS) << ((9 * place) // EXPERTS)) // EXPERTS
    wait = (jax.random.bits(ke, (*devices, TOKENS, EXPERTS), jnp.uint32) >> 10) * slow
    expert = jnp.argsort(wait, axis=-1)[..., :TOP].astype(jnp.int32)
    chosen = jax.nn.one_hot(expert, EXPERTS, dtype=jnp.int32)
    in_line = jnp.cumsum(chosen.reshape(*devices, TOKENS * TOP, EXPERTS), axis=2) - 1
    slot = jnp.sum(in_line.reshape(chosen.shape) * chosen, axis=-1)

    def one(key, rows, columns):
        return (jax.random.normal(key, (rows, columns), jnp.float32) * rows**-0.5).astype(jnp.bfloat16)

    def weights(key, rows, columns):
        return jax.lax.map(lambda k: one(k, rows, columns), jax.random.split(key, EXPERTS))

    return {
        "x": jax.random.normal(kx, (*devices, TOKENS, D), jnp.float32).astype(jnp.bfloat16),
        "expert": expert,
        "slot": slot,
        "gate": jax.nn.softmax(jax.random.normal(kg, expert.shape, jnp.float32)),
        "w_gate": weights(k1, D, FF),
        "w_up": weights(k2, D, FF),
        "w_down": weights(k3, FF, D),
        "s_gate": one(k4, D, SHARED_FF),
        "s_up": one(k5, D, SHARED_FF),
        "s_down": one(k6, SHARED_FF, D),
    }


def einsum(form, a, b):
    return jnp.einsum(form, a.astype(jnp.float32), b.astype(jnp.float32))


def for_all(x, s_gate, s_up, s_down):
    h = jax.nn.silu(einsum("...d,df->...f", x, s_gate)) * einsum("...d,df->...f", x, s_up)
    return einsum("...f,fd->...d", h.astype(jnp.bfloat16), s_down)


def reference(x, expert, slot, gate, w_gate, w_up, w_down, s_gate, s_up, s_down):
    to_expert = jax.nn.one_hot(expert, EXPERTS, dtype=jnp.bfloat16)
    to_slot = jax.nn.one_hot(slot, SLOTS, dtype=jnp.bfloat16)
    weighted = to_expert * gate[..., None].astype(jnp.bfloat16)
    dispatch = einsum("abtke,abtkc->abtec", to_expert, to_slot).astype(jnp.bfloat16)
    combine = einsum("abtke,abtkc->abtec", weighted, to_slot).astype(jnp.bfloat16)
    z = einsum("abtec,abtd->aebcd", dispatch, x).astype(jnp.bfloat16)
    h = jax.nn.silu(einsum("aebcd,edf->aebcf", z, w_gate))
    h = (h * einsum("aebcd,edf->aebcf", z, w_up)).astype(jnp.bfloat16)
    out = einsum("aebcf,efd->aebcd", h, w_down).astype(jnp.bfloat16)
    y = einsum("abtec,aebcd->abtd", combine, out)
    return (y + for_all(x, s_gate, s_up, s_down)).astype(jnp.bfloat16)
```

```python
import functools
import math

import jax
import jax.numpy as jnp
from jax import lax
from jax.experimental import pallas as pl
from jax.experimental.pallas import tpu as pltpu
from jax.sharding import PartitionSpec as P

F32, BF16 = jnp.float32, jnp.bfloat16
LO, HI = 16, 8
CT = 256
DB = 4


def dot(a, b):
    return jnp.dot(a, b, preferred_element_type=F32)


def cols(i):
    return pl.ds(pl.multiple_of(i * CT, CT), CT)


def kernel(
    S, EPD, TOP,
    x_ref, meta_ref, wg, wu, wd, sg, su, sd, y_ref,
    ag, mall, oh, dsend, z, zf, crecv, via, fin, cmat, h, ysh, gu, db,
    gu_sem, db_sem, ag_s, ag_r, m_s, m_r, z_s, z_r, c_s, c_r, v_s, v_r, f_s, f_r,
):
    T, D = x_ref.shape
    FF = wg.shape[2]
    H = D // 2
    SL = LO + HI
    CH = S * SL
    HT = T // 2
    QS = sg.shape[1] // FF
    NG, NDT = FF // CT, D // CT
    HTILES = H // CT
    me = lax.axis_index("ep")
    px, py = lax.div(me, S), lax.rem(me, S)

    def dev(p, df, ds):
        dx = df * (1 - p) + ds * p
        dy = df * p + ds * (1 - p)
        return lax.rem(px + dx, S) * S + lax.rem(py + dy, S)

    def start_gu(n):
        slot = lax.rem(n, 2)

        @pl.when(n < QS * NG)
        def _():
            c = cols(n)
            pltpu.make_async_copy(sg.at[:, c], gu.at[slot, 0], gu_sem.at[slot, 0]).start()
            pltpu.make_async_copy(su.at[:, c], gu.at[slot, 1], gu_sem.at[slot, 1]).start()

        @pl.when(jnp.logical_and(n >= QS * NG, n < (QS + EPD) * NG))
        def _():
            k = n - QS * NG
            e, c = lax.div(k, NG), cols(lax.rem(k, NG))
            pltpu.make_async_copy(wg.at[e, :, c], gu.at[slot, 0], gu_sem.at[slot, 0]).start()
            pltpu.make_async_copy(wu.at[e, :, c], gu.at[slot, 1], gu_sem.at[slot, 1]).start()

    def wait_gu(n):
        slot = lax.rem(n, 2)
        for j in range(2):
            pltpu.make_async_copy(sg.at[:, cols(0)], gu.at[slot, j], gu_sem.at[slot, j]).wait()
        return slot

    def start_db(m):
        slot = lax.rem(m, DB)

        @pl.when(m < QS * NDT)
        def _():
            q, c = lax.div(m, NDT), cols(lax.rem(m, NDT))
            rows = pl.ds(pl.multiple_of(q * FF, FF), FF)
            pltpu.make_async_copy(sd.at[rows, c], db.at[slot], db_sem.at[slot]).start()

        @pl.when(jnp.logical_and(m >= QS * NDT, m < (QS + EPD) * NDT))
        def _():
            k = m - QS * NDT
            pltpu.make_async_copy(
                wd.at[lax.div(k, NDT), :, cols(lax.rem(k, NDT))], db.at[slot], db_sem.at[slot]
            ).start()

    def wait_db(m):
        slot = lax.rem(m, DB)
        pltpu.make_async_copy(wd.at[0, :, cols(0)], db.at[slot], db_sem.at[slot]).wait()
        return slot

    start_gu(jnp.int32(0))
    for m in range(DB - 1):
        start_db(jnp.int32(m))

    barrier = pltpu.get_barrier_semaphore()
    for p in range(2):
        for d in range(1, S):
            pl.semaphore_signal(barrier, inc=1, device_id={"ep": dev(p, d, 0)})
    pl.semaphore_wait(barrier, 2 * (S - 1))

    def remote(src, dst, s, r, to):
        return pltpu.make_async_remote_copy(src, dst, s, r, device_id={"ep": to})

    def xcols(p):
        return x_ref.at[:, pl.ds(p * H, H)]

    def meta_copy(p, d):
        return remote(meta_ref, mall.at[p, S - d], m_s.at[p, d - 1], m_r.at[p, S - d - 1], dev(p, d, 0))

    def ag_first(p, d):
        i = 0 if d == 1 else 1
        return remote(xcols(p), ag.at[p, S - d - 1], ag_s.at[p, i], ag_r.at[p, i], dev(p, d, 0))

    def ag_relay(p, d):
        i = 0 if d == 1 else 1
        src = ag.at[p, (S - 1 if d == 1 else 1) - 1, pl.ds(i * HT, HT)]
        dst = ag.at[p, 2 - 1, pl.ds(i * HT, HT)]
        return remote(src, dst, ag_s.at[p, 2 + i], ag_r.at[p, 2 + i], dev(p, d, 0))

    for p in range(2):
        for d in range(1, S):
            meta_copy(p, d).start()
        for d in (1, S - 1):
            ag_first(p, d).start()
    for p in range(2):
        mall[p, 0] = meta_ref[...]

    def ffn_tile(lhs, rows, n, i):
        slot = wait_gu(n)
        start_gu(n + 1)
        g = dot(lhs, gu[slot, 0])
        u = dot(lhs, gu[slot, 1])
        h[0:rows, cols(i)] = (jax.nn.silu(g) * u).astype(BF16)

    for q in range(QS):

        def up(i, _):
            ffn_tile(x_ref[...], T, q * NG + i, i)
            return 0

        lax.fori_loop(0, NG, up, 0)

        def down(c, _):
            m = q * NDT + c
            slot = wait_db(m)
            start_db(m + DB - 1)
            o = dot(h[0:T, :], db[slot])
            ysh[:, cols(c)] = o if q == 0 else ysh[:, cols(c)] + o
            return 0

        lax.fori_loop(0, NDT, down, 0)

    for p in range(2):
        ag_first(p, 1).wait_recv()
        ag_relay(p, 1).start()
        ag_first(p, S - 1).wait_recv()
        ag_relay(p, S - 1).start()
    for p in range(2):
        for d in range(1, S):
            meta_copy(p, d).wait_recv()

    def source(p, r, c):
        if r == 0:
            return x_ref[:, pl.ds(pl.multiple_of(p * H + c * CT, CT), CT)]
        return ag[p, r - 1, :, cols(c)]

    def onehot(p, r):
        i = lax.broadcasted_iota(jnp.int32, (S * EPD * SL, T), 0)
        n = EPD * SL
        off = dev(p, 0, S - 1) * n - (S - 1) * n
        for k in range(S - 2, -1, -1):
            off = jnp.where(i < (k + 1) * n, (dev(p, 0, k) - k) * n, off)
        code = (i + off).astype(F32)
        total = jnp.zeros(code.shape, F32)
        for j in range(TOP):
            total += jnp.where(code == mall[p, r, j : j + 1, :], 1.0, 0.0)
        return total.astype(BF16)

    def select(p, pair):
        for j in range(2):
            oh[j] = onehot(p, 2 * pair + j)

        def tile(c, _):
            a = dot(oh[0], source(p, 2 * pair, c))
            b = dot(oh[1], source(p, 2 * pair + 1, c))
            for k in range(S):
                for e in range(EPD):
                    o = (k * EPD + e) * SL
                    lo = jnp.concatenate([a[o : o + LO], b[o : o + LO]], 0).astype(BF16)
                    hi = jnp.concatenate([a[o + LO : o + SL], b[o + LO : o + SL]], 0).astype(BF16)
                    l0, h0 = pair * 2 * LO, S * LO + pair * 2 * HI
                    if k == 0:
                        z[p, e, 0, l0 : l0 + 2 * LO, cols(c)] = lo
                        z[p, e, 0, h0 : h0 + 2 * HI, cols(c)] = hi
                    else:
                        dsend[p, k - 1, e * CH + l0 : e * CH + l0 + 2 * LO, cols(c)] = lo
                        dsend[p, k - 1, e * CH + h0 : e * CH + h0 + 2 * HI, cols(c)] = hi
            return 0

        lax.fori_loop(0, HTILES, tile, 0)

    for p in range(2):
        select(p, 0)
    for p in range(2):
        for d in (1, S - 1):
            ag_relay(p, d).wait_recv()
    for p in range(2):
        select(p, 1)

    def z_copy(p, e, k):
        rows = pl.ds(e * CH, CH) if isinstance(e, int) else pl.ds(pl.multiple_of(e * CH, CH), CH)
        return remote(
            dsend.at[p, k - 1, rows], z.at[p, e, S - k],
            z_s.at[p, e, k - 1], z_r.at[p, e, S - k - 1], dev(p, 0, k),
        )

    for e in range(EPD):
        for k in (1, S - 1, 2):
            for p in range(2):
                z_copy(p, e, k).start()

    def coefficients(n, _):
        p, r = lax.div(n, S), lax.rem(n, S)
        half = EPD * S * LO
        i = lax.broadcasted_iota(jnp.int32, (2 * half, T), 0)
        high = i >= half
        i = jnp.where(high, i - half, i)
        e, kk, c = i >> 6, (i >> 4) & 3, i & 15
        owner = jnp.where(kk == 0, dev(p, 0, 0), 0)
        for k in range(1, S):
            owner = jnp.where(kk == k, dev(p, 0, k), owner)
        odd = c >> 3
        slot = jnp.where(high, LO + (c & 7), c)
        code = (owner * EPD + e) * SL + slot
        code = jnp.where(jnp.logical_and(high, odd != lax.rem(r, 2)), -2, code).astype(F32)
        total = jnp.zeros(code.shape, F32)
        for j in range(TOP):
            total += jnp.where(code == mall[p, r, j : j + 1, :], mall[p, r, 8 + j : 9 + j, :], 0.0)
        cmat[p, r] = total.T.astype(BF16)
        return 0

    lax.fori_loop(0, 2 * S, coefficients, 0)

    def c_copy(p, e, k):
        return remote(
            z.at[p, e, k], crecv.at[p, e, S - k],
            c_s.at[p, e, k - 1], c_r.at[p, e, S - k - 1], dev(p, 0, k),
        )

    def expert(e, _):
        for k in (1, S - 1, 2):
            for p in range(2):
                z_copy(p, e, k).wait_recv()
        for k in range(S):
            zf[k * CH : (k + 1) * CH, 0:H] = z[0, e, k]
            for r in range(S):
                o = k * CH + r * LO
                zf[o : o + LO, H:D] = z[1, e, r, k * LO : (k + 1) * LO]
            u0 = S * LO + (k // 2) * 2 * HI
            for r in range(0, S, 2):
                o = k * CH + S * LO + r * HI
                part = [
                    z[1, e, r + j, u0 : u0 + 2 * HI].astype(F32)[(k % 2) * HI : (k % 2 + 1) * HI]
                    for j in range(2)
                ]
                zf[o : o + 2 * HI, H:D] = jnp.concatenate(part, 0).astype(BF16)

        def up(i, _):
            ffn_tile(zf[...], S * CH, (QS + e) * NG + i, i)
            return 0

        lax.fori_loop(0, NG, up, 0)

        for p in range(2):

            def down(c, _):
                m = (QS + e) * NDT + p * HTILES + c
                slot = wait_db(m)
                start_db(m + DB - 1)
                o = dot(h[...], db[slot])
                for k in range(S):
                    if p == 0:
                        b = o[k * CH : (k + 1) * CH]
                    else:
                        low = [o[r * CH + k * LO : r * CH + (k + 1) * LO] for r in range(S)]
                        n = S * LO + k * HI
                        high = [o[r * CH + n : r * CH + n + HI] for r in range(S)]
                        b = jnp.concatenate(low + high, 0)
                    if k == 0:
                        crecv[p, e, 0, :, cols(c)] = b.astype(BF16)
                    else:
                        z[p, e, k, :, cols(c)] = b.astype(BF16)
                return 0

            lax.fori_loop(0, HTILES, down, 0)
            for k in (1, S - 1, 2):
                c_copy(p, e, k).start()
        return 0

    lax.fori_loop(0, EPD, expert, 0)

    for p in range(2):
        for e in range(EPD):
            for k in range(1, S):
                z_copy(p, e, k).wait_send()

    def slots(p, r, c):
        a = crecv[p, :, :, r * LO : (r + 1) * LO, cols(c)].reshape(EPD * S * LO, CT)
        u0 = S * LO + (r // 2) * 2 * HI
        b = crecv[p, :, :, u0 : u0 + 2 * HI, cols(c)].reshape(EPD * S * LO, CT)
        return jnp.concatenate([a, b], 0)

    def part(p, r, c, r0, r1):
        return dot(cmat[p, r, r0:r1], slots(p, r, c))

    def via_copy(p, i):
        src = dsend.at[p, 1, pl.ds(i * HT, HT)]
        return remote(src, via.at[p, i], v_s.at[p, i], v_r.at[p, i], dev(p, 1 if i == 0 else S - 1, 0))

    def fin_copy(p, i, half):
        src = dsend.at[p, 2 * i, pl.ds(half * HT, HT)]
        dst = fin.at[p, i, pl.ds(half * HT, HT)]
        return remote(src, dst, f_s.at[p, i, half], f_r.at[p, i, half], dev(p, 1 if i == 0 else S - 1, 0))

    for p in range(2):
        for e in range(EPD):
            for k in range(1, S):
                c_copy(p, e, k).wait_recv()

        def far(c, _):
            dsend[p, 1, 0:T, cols(c)] = part(p, 2, c, 0, T).astype(BF16)
            return 0

        lax.fori_loop(0, HTILES, far, 0)
        for i in range(2):
            via_copy(p, i).start()

    for p in range(2):

        def near(c, _):
            dsend[p, 0, HT:T, cols(c)] = part(p, 1, c, HT, T).astype(BF16)
            dsend[p, 2, 0:HT, cols(c)] = part(p, S - 1, c, 0, HT).astype(BF16)
            return 0

        lax.fori_loop(0, HTILES, near, 0)
        fin_copy(p, 0, 1).start()
        fin_copy(p, 1, 0).start()

    for p in range(2):
        for i in range(2):
            via_copy(p, i).wait_recv()

        def through(c, _):
            a = part(p, 1, c, 0, HT) + via[p, 0, :, cols(c)].astype(F32)
            b = part(p, S - 1, c, HT, T) + via[p, 1, :, cols(c)].astype(F32)
            dsend[p, 0, 0:HT, cols(c)] = a.astype(BF16)
            dsend[p, 2, HT:T, cols(c)] = b.astype(BF16)
            return 0

        lax.fori_loop(0, HTILES, through, 0)
        fin_copy(p, 0, 0).start()
        fin_copy(p, 1, 1).start()

    for p in range(2):

        def own(c, _):
            ysh[:, cols(p * HTILES + c)] += part(p, 0, c, 0, T)
            return 0

        lax.fori_loop(0, HTILES, own, 0)

    for p in range(2):
        for i in range(2):
            for half in range(2):
                fin_copy(p, i, half).wait_recv()

        def last(c, _):
            a = fin[p, 0, :, cols(c)].astype(F32) + fin[p, 1, :, cols(c)].astype(F32)
            at = cols(p * HTILES + c)
            y_ref[:, at] = (ysh[:, at] + a).astype(y_ref.dtype)
            return 0

        lax.fori_loop(0, HTILES, last, 0)

    for p in range(2):
        for d in range(1, S):
            meta_copy(p, d).wait_send()
        for d in (1, S - 1):
            ag_first(p, d).wait_send()
            ag_relay(p, d).wait_send()
        for e in range(EPD):
            for k in range(1, S):
                c_copy(p, e, k).wait_send()
        for i in range(2):
            via_copy(p, i).wait_send()
            for half in range(2):
                fin_copy(p, i, half).wait_send()


def solution(mesh):
    side = math.isqrt(mesh.shape["ep"])

    def local(x, expert, slot, gate, w_gate, w_up, w_down, s_gate, s_up, s_down):
        T, D = x.shape[2:]
        TOP = expert.shape[3]
        EPD, _, FF = w_gate.shape
        SL, S, H = LO + HI, side, D // 2
        assert side * side == mesh.shape["ep"] and side == 4
        assert SL == 5 * T * TOP // (4 * EPD * mesh.shape["ep"])
        code = jnp.where(slot < SL, expert * SL + slot, -1).astype(F32).reshape(T, TOP)
        meta = jnp.pad(
            jnp.stack([code.T, gate.reshape(T, TOP).T]), ((0, 0), (0, 8 - TOP), (0, 0))
        ).reshape(16, T)
        rows = EPD * S * SL
        sem = pltpu.SemaphoreType.DMA
        y = pl.pallas_call(
            functools.partial(kernel, S, EPD, TOP),
            out_shape=jax.ShapeDtypeStruct((T, D), x.dtype),
            in_specs=[pl.BlockSpec(memory_space=pltpu.VMEM)] * 2
            + [pl.BlockSpec(memory_space=pl.ANY)] * 6,
            out_specs=pl.BlockSpec(memory_space=pltpu.VMEM),
            scratch_shapes=[
                pltpu.VMEM((2, S - 1, T, H), BF16),
                pltpu.VMEM((2, S, 16, T), F32),
                pltpu.VMEM((2, rows, T), BF16),
                pltpu.VMEM((2, S - 1, rows, H), BF16),
                pltpu.VMEM((2, EPD, S, S * SL, H), BF16),
                pltpu.VMEM((S * S * SL, D), BF16),
                pltpu.VMEM((2, EPD, S, S * SL, H), BF16),
                pltpu.VMEM((2, 2, T // 2, H), BF16),
                pltpu.VMEM((2, 2, T, H), BF16),
                pltpu.VMEM((2, S, T, 2 * EPD * S * LO), BF16),
                pltpu.VMEM((S * S * SL, FF), BF16),
                pltpu.VMEM((T, D), F32),
                pltpu.VMEM((2, 2, D, CT), BF16),
                pltpu.VMEM((DB, FF, CT), BF16),
                sem((2, 2)), sem((DB,)),
                sem((2, 4)), sem((2, 4)),
                sem((2, S - 1)), sem((2, S - 1)),
                sem((2, EPD, S - 1)), sem((2, EPD, S - 1)),
                sem((2, EPD, S - 1)), sem((2, EPD, S - 1)),
                sem((2, 2)), sem((2, 2)),
                sem((2, 2, 2)), sem((2, 2, 2)),
            ],
            compiler_params=pltpu.CompilerParams(
                collective_id=0, has_side_effects=True, vmem_limit_bytes=67043328
            ),
        )(x.reshape(T, D), meta, w_gate, w_up, w_down, s_gate, s_up, s_down)
        return y.reshape(x.shape)

    own, experts, whole = P("dp", "ep"), P("ep"), P()
    return jax.shard_map(
        local,
        mesh=mesh,
        in_specs=(own,) * 4 + (experts,) * 3 + (whole,) * 3,
        out_specs=own,
        check_vma=False,
    )
```

```python
import functools
import math

import jax
import jax.numpy as jnp
from jax import lax
from jax.experimental import pallas as pl
from jax.experimental.pallas import tpu as pltpu
from jax.sharding import PartitionSpec as P

F32, BF16 = jnp.float32, jnp.bfloat16
LO, HI = 16, 8
CT = 256
DB = 4
EARLY = 1


def dot(a, b):
    return jnp.dot(a, b, preferred_element_type=F32)


def cols(i):
    return pl.ds(pl.multiple_of(i * CT, CT), CT)


def kernel(
    S, EPD, TOP,
    x_hbm, expert_ref, slot_ref, gate_ref, wg, wu, wd, sg, su, sd, y_ref,
    x_ref, meta_ref, flip, ag, mall, oh, dsend, z, zf, crecv, via, fin, cmat, h, ysh, gu, db,
    x_sem, gu_sem, db_sem, ag_s, ag_r, m_s, m_r, z_s, z_r, c_s, c_r, v_s, v_r, f_s, f_r,
):
    T, D = x_ref.shape
    FF = wg.shape[2]
    H = D // 2
    SL = LO + HI
    CH = S * SL
    HT = T // 2
    PR = 2 * SL
    LAST = EPD + 1
    NG, NDT = FF // CT, D // CT
    HTILES = H // CT
    me = lax.axis_index("ep")
    px, py = lax.div(me, S), lax.rem(me, S)

    def dev(p, df, ds):
        dx = df * (1 - p) + ds * p
        dy = df * p + ds * (1 - p)
        return lax.rem(px + dx, S) * S + lax.rem(py + dy, S)

    def lo(r):
        return (r // 2) * PR + (r % 2) * LO

    def hi(r):
        return (r // 2) * PR + 2 * LO + (r % 2) * HI

    def start_gu(n):
        slot = lax.rem(n, 2)
        u, c = lax.div(n, NG), lax.rem(n, NG)

        @pl.when(jnp.logical_or(u == 0, u == LAST))
        def _():
            at = cols(c + lax.div(u, LAST) * NG)
            pltpu.make_async_copy(sg.at[:, at], gu.at[slot, 0], gu_sem.at[slot, 0]).start()
            pltpu.make_async_copy(su.at[:, at], gu.at[slot, 1], gu_sem.at[slot, 1]).start()

        @pl.when(jnp.logical_and(u > 0, u < LAST))
        def _():
            pltpu.make_async_copy(wg.at[u - 1, :, cols(c)], gu.at[slot, 0], gu_sem.at[slot, 0]).start()
            pltpu.make_async_copy(wu.at[u - 1, :, cols(c)], gu.at[slot, 1], gu_sem.at[slot, 1]).start()

    def wait_gu(n):
        slot = lax.rem(n, 2)
        for j in range(2):
            pltpu.make_async_copy(sg.at[:, cols(0)], gu.at[slot, j], gu_sem.at[slot, j]).wait()
        return slot

    def start_db(m):
        slot = lax.rem(m, DB)
        u, c = lax.div(m, NDT), lax.rem(m, NDT)

        @pl.when(jnp.logical_or(u == 0, u == LAST))
        def _():
            rows = pl.ds(pl.multiple_of(lax.div(u, LAST) * FF, FF), FF)
            pltpu.make_async_copy(sd.at[rows, cols(c)], db.at[slot], db_sem.at[slot]).start()

        @pl.when(jnp.logical_and(u > 0, u < LAST))
        def _():
            pltpu.make_async_copy(wd.at[u - 1, :, cols(c)], db.at[slot], db_sem.at[slot]).start()

    def wait_db(m):
        slot = lax.rem(m, DB)
        pltpu.make_async_copy(wd.at[0, :, cols(0)], db.at[slot], db_sem.at[slot]).wait()
        return slot

    x_copy = pltpu.make_async_copy(x_hbm, x_ref, x_sem)
    x_copy.start()
    start_gu(jnp.int32(0))
    for m in range(DB - 1):
        start_db(jnp.int32(m))

    barrier = pltpu.get_barrier_semaphore()
    for p in range(2):
        for d in range(1, S):
            pl.semaphore_signal(barrier, inc=1, device_id={"ep": dev(p, d, 0)})
    pl.semaphore_wait(barrier, 2 * (S - 1))

    def remote(src, dst, s, r, to):
        return pltpu.make_async_remote_copy(src, dst, s, r, device_id={"ep": to})

    def ag_first(p, d, early):
        i = 0 if d == 1 else 1
        rows = pl.ds((i if early else 1 - i) * HT, HT)
        n = i if early else 2 + i
        return remote(
            x_hbm.at[rows, pl.ds(p * H, H)], ag.at[p, S - d - 1, rows],
            ag_s.at[p, n], ag_r.at[p, n], dev(p, d, 0),
        )

    def ag_relay(p, d):
        i = 0 if d == 1 else 1
        rows = pl.ds(i * HT, HT)
        src = ag.at[p, (S - 1 if d == 1 else 1) - 1, rows]
        return remote(src, ag.at[p, 1, rows], ag_s.at[p, 4 + i], ag_r.at[p, 4 + i], dev(p, d, 0))

    def meta_copy(p, d):
        return remote(meta_ref, mall.at[p, S - d], m_s.at[p, d - 1], m_r.at[p, S - d - 1], dev(p, d, 0))

    for early in (True, False):
        for p in range(2):
            for d in (1, S - 1):
                ag_first(p, d, early).start()

    flip[...] = jnp.zeros(flip.shape, F32)
    slot = slot_ref[...]
    flip[0, :, 0:TOP] = jnp.where(slot < SL, expert_ref[...] * SL + slot, -1).astype(F32)
    flip[1, :, 0:TOP] = gate_ref[...]
    meta_ref[0:8] = flip[0].T[0:8]
    meta_ref[8:16] = flip[1].T[0:8]
    for p in range(2):
        mall[p, 0] = meta_ref[...]
        for d in range(1, S):
            meta_copy(p, d).start()

    def up(lhs, rows, u):
        def tile(i, _):
            n = u * NG + i
            slot = wait_gu(n)
            pl.when(n + 1 < (LAST + 1) * NG)(lambda: start_gu(n + 1))
            g = dot(lhs[...], gu[slot, 0])
            v = dot(lhs[...], gu[slot, 1])
            h[0:rows, cols(i)] = (jax.nn.silu(g) * v).astype(BF16)
            return 0

        lax.fori_loop(0, NG, tile, 0)

    def down_tile(rows, u, c):
        m = u * NDT + c
        slot = wait_db(m)
        pl.when(m + DB - 1 < (LAST + 1) * NDT)(lambda: start_db(m + DB - 1))
        return dot(h[0:rows, :], db[slot])

    def shared_down(u):
        def tile(c, _):
            o = down_tile(T, u, c)
            ysh[:, cols(c)] = o if u == 0 else ysh[:, cols(c)] + o
            return 0

        lax.fori_loop(0, NDT, tile, 0)

    x_copy.wait()
    up(x_ref, T, 0)
    for p in range(2):
        for d in (1, S - 1):
            ag_first(p, d, True).wait_recv()
        ag_relay(p, 1).start()
        ag_relay(p, S - 1).start()
    shared_down(0)

    for p in range(2):
        for d in (1, S - 1):
            ag_first(p, d, False).wait_recv()
        for d in range(1, S):
            meta_copy(p, d).wait_recv()

    def source(p, r, c):
        if r == 0:
            return x_ref[:, pl.ds(pl.multiple_of(p * H + c * CT, CT), CT)]
        return ag[p, r - 1, :, cols(c)]

    def onehot(p, r):
        i = lax.broadcasted_iota(jnp.int32, (S * EPD * SL, T), 0)
        n = EPD * SL
        off = dev(p, 0, S - 1) * n - (S - 1) * n
        for k in range(S - 2, -1, -1):
            off = jnp.where(i < (k + 1) * n, (dev(p, 0, k) - k) * n, off)
        code = (i + off).astype(F32)
        total = jnp.zeros(code.shape, F32)
        for j in range(TOP):
            total += jnp.where(code == mall[p, r, j : j + 1, :], 1.0, 0.0)
        return total.astype(BF16)

    def select(p, pair):
        for j in range(2):
            oh[j] = onehot(p, 2 * pair + j)

        def tile(c, _):
            a = dot(oh[0], source(p, 2 * pair, c))
            b = dot(oh[1], source(p, 2 * pair + 1, c))
            for k in range(S):
                for e in range(EPD):
                    o = (k * EPD + e) * SL
                    m = o + LO
                    b48 = jnp.concatenate([a[o:m], b[o:m], a[m : o + SL], b[m : o + SL]], 0)
                    at = pair * PR
                    if k == 0:
                        z[p, e, 0, at : at + PR, cols(c)] = b48.astype(BF16)
                    else:
                        at += e * CH
                        dsend[p, k - 1, at : at + PR, cols(c)] = b48.astype(BF16)
            return 0

        lax.fori_loop(0, HTILES, tile, 0)

    def halves(e):
        return (0, 1) if e < EARLY else (2,)

    def z_copy(p, e, k, half):
        at, n = (half * PR, PR) if half < 2 else (0, CH)
        rows = pl.ds(pl.multiple_of(e * CH + at, PR), n)
        return remote(
            dsend.at[p, k - 1, rows], z.at[p, e, S - k, pl.ds(at, n)],
            z_s.at[p, e, k - 1, half % 2], z_r.at[p, e, S - k - 1, half % 2], dev(p, 0, k),
        )

    def z_start(e, half):
        for k in (1, S - 1, 2):
            for p in range(2):
                z_copy(p, e, k, half).start()

    for p in range(2):
        select(p, 0)
    for e in range(EARLY):
        z_start(e, 0)
    for p in range(2):
        for d in (1, S - 1):
            ag_relay(p, d).wait_recv()
    for p in range(2):
        select(p, 1)
    for e in range(EPD):
        z_start(e, 1 if e < EARLY else 2)

    def coefficients(n, _):
        p, r = lax.div(n, S), lax.rem(n, S)
        half = EPD * S * LO
        i = lax.broadcasted_iota(jnp.int32, (2 * half, T), 0)
        high = i >= half
        i = jnp.where(high, i - half, i)
        e, kk, c = i >> 6, (i >> 4) & 3, i & 15
        owner = jnp.where(kk == 0, dev(p, 0, 0), 0)
        for k in range(1, S):
            owner = jnp.where(kk == k, dev(p, 0, k), owner)
        odd = c >> 3
        slot = jnp.where(high, LO + (c & 7), c)
        code = (owner * EPD + e) * SL + slot
        code = jnp.where(jnp.logical_and(high, odd != lax.rem(r, 2)), -2, code).astype(F32)
        total = jnp.zeros(code.shape, F32)
        for j in range(TOP):
            total += jnp.where(code == mall[p, r, j : j + 1, :], mall[p, r, 8 + j : 9 + j, :], 0.0)
        cmat[p, r] = total.T.astype(BF16)
        return 0

    lax.fori_loop(0, 2 * S, coefficients, 0)

    def c_copy(p, e, k, half):
        at, n = (half * PR, PR) if half < 2 else (0, CH)
        return remote(
            z.at[p, e, k, pl.ds(at, n)], crecv.at[p, e, S - k, pl.ds(at, n)],
            c_s.at[p, e, k - 1, half % 2], c_r.at[p, e, S - k - 1, half % 2], dev(p, 0, k),
        )

    def expert(e, _):
        def arrived(half):
            for k in (1, S - 1, 2):
                for p in range(2):
                    z_copy(p, e, k, half).wait_recv()

        @pl.when(e < EARLY)
        def _():
            arrived(0)
            arrived(1)

        @pl.when(e >= EARLY)
        def _():
            arrived(2)

        for k in range(S):
            zf[k * CH : (k + 1) * CH, 0:H] = z[0, e, k]
            for r in range(S):
                o = k * CH + lo(r)
                zf[o : o + LO, H:D] = z[1, e, r, lo(k) : lo(k) + LO]
            u0 = hi(k) - (k % 2) * HI
            for r in range(0, S, 2):
                o = k * CH + hi(r)
                two = [
                    z[1, e, r + j, u0 : u0 + 2 * HI].astype(F32)[(k % 2) * HI : (k % 2 + 1) * HI]
                    for j in range(2)
                ]
                zf[o : o + 2 * HI, H:D] = jnp.concatenate(two, 0).astype(BF16)

        up(zf, S * CH, 1 + e)

        def back(p, half):
            for k in (1, S - 1, 2):
                c_copy(p, e, k, half).start()

        for p in range(2):

            def tile(c, _):
                o = down_tile(S * CH, 1 + e, p * HTILES + c)
                for k in range(S):
                    if p == 0:
                        b = o[k * CH : (k + 1) * CH]
                    else:
                        rows = []
                        for r in range(0, S, 2):
                            for f, n in ((lo(k), LO), (hi(k), HI)):
                                rows += [o[q * CH + f : q * CH + f + n] for q in (r, r + 1)]
                        b = jnp.concatenate(rows, 0)
                    if k == 0:
                        crecv[p, e, 0, :, cols(c)] = b.astype(BF16)
                    else:
                        z[p, e, k, :, cols(c)] = b.astype(BF16)
                return 0

            lax.fori_loop(0, HTILES, tile, 0)
            pl.when(e < EPD - 1)(lambda: back(p, 2))

        @pl.when(e == EPD - 1)
        def _():
            for half in (1, 0):
                for p in range(2):
                    back(p, half)

        return 0

    lax.fori_loop(0, EPD, expert, 0)
    up(x_ref, T, LAST)
    shared_down(LAST)

    for p in range(2):
        for e in range(EPD):
            for k in range(1, S):
                for half in halves(e):
                    z_copy(p, e, k, half).wait_send()

    def slots(p, r, c):
        a = crecv[p, :, :, lo(r) : lo(r) + LO, cols(c)].reshape(EPD * S * LO, CT)
        u0 = hi(r) - (r % 2) * HI
        b = crecv[p, :, :, u0 : u0 + 2 * HI, cols(c)].reshape(EPD * S * LO, CT)
        return jnp.concatenate([a, b], 0)

    def part(p, r, c, r0, r1):
        return dot(cmat[p, r, r0:r1], slots(p, r, c))

    def via_copy(p, i):
        src = dsend.at[p, 1, pl.ds(i * HT, HT)]
        return remote(src, via.at[p, i], v_s.at[p, i], v_r.at[p, i], dev(p, 1 if i == 0 else S - 1, 0))

    def fin_copy(p, i, half):
        src = dsend.at[p, 2 * i, pl.ds(half * HT, HT)]
        dst = fin.at[p, i, pl.ds(half * HT, HT)]
        return remote(src, dst, f_s.at[p, i, half], f_r.at[p, i, half], dev(p, 1 if i == 0 else S - 1, 0))

    for p in range(2):
        for e in range(EPD):
            for k in range(1, S):
                c_copy(p, e, k, 2 if e < EPD - 1 else 1).wait_recv()

        def far(c, _):
            dsend[p, 1, 0:T, cols(c)] = part(p, 2, c, 0, T).astype(BF16)
            return 0

        lax.fori_loop(0, HTILES, far, 0)
        for i in range(2):
            via_copy(p, i).start()

    for p in range(2):

        def before(c, _):
            dsend[p, 2, 0:HT, cols(c)] = part(p, S - 1, c, 0, HT).astype(BF16)
            return 0

        lax.fori_loop(0, HTILES, before, 0)
        fin_copy(p, 1, 0).start()

    for p in range(2):
        for k in range(1, S):
            c_copy(p, EPD - 1, k, 0).wait_recv()

        def after(c, _):
            dsend[p, 0, HT:T, cols(c)] = part(p, 1, c, HT, T).astype(BF16)
            return 0

        lax.fori_loop(0, HTILES, after, 0)
        fin_copy(p, 0, 1).start()

    for p in range(2):
        for i in range(2):
            via_copy(p, i).wait_recv()

        def through(c, _):
            a = part(p, 1, c, 0, HT) + via[p, 0, :, cols(c)].astype(F32)
            b = part(p, S - 1, c, HT, T) + via[p, 1, :, cols(c)].astype(F32)
            dsend[p, 0, 0:HT, cols(c)] = a.astype(BF16)
            dsend[p, 2, HT:T, cols(c)] = b.astype(BF16)
            return 0

        lax.fori_loop(0, HTILES, through, 0)
        fin_copy(p, 0, 0).start()
        fin_copy(p, 1, 1).start()

    for p in range(2):

        def own(c, _):
            ysh[:, cols(p * HTILES + c)] += part(p, 0, c, 0, T)
            return 0

        lax.fori_loop(0, HTILES, own, 0)

    for p in range(2):
        for i in range(2):
            for half in range(2):
                fin_copy(p, i, half).wait_recv()

        def last(c, _):
            a = fin[p, 0, :, cols(c)].astype(F32) + fin[p, 1, :, cols(c)].astype(F32)
            at = cols(p * HTILES + c)
            y_ref[:, at] = (ysh[:, at] + a).astype(y_ref.dtype)
            return 0

        lax.fori_loop(0, HTILES, last, 0)

    for p in range(2):
        for d in range(1, S):
            meta_copy(p, d).wait_send()
        for d in (1, S - 1):
            for early in (True, False):
                ag_first(p, d, early).wait_send()
            ag_relay(p, d).wait_send()
        for e in range(EPD):
            for k in range(1, S):
                for half in (2,) if e < EPD - 1 else (0, 1):
                    c_copy(p, e, k, half).wait_send()
        for i in range(2):
            via_copy(p, i).wait_send()
            for half in range(2):
                fin_copy(p, i, half).wait_send()


def solution(mesh):
    side = math.isqrt(mesh.shape["ep"])

    def local(x, expert, slot, gate, w_gate, w_up, w_down, s_gate, s_up, s_down):
        T, D = x.shape[2:]
        TOP = expert.shape[3]
        EPD, _, FF = w_gate.shape
        SL, S, H = LO + HI, side, D // 2
        assert side * side == mesh.shape["ep"] and side == 4
        assert FF * 2 == s_gate.shape[1] and SL == 5 * T * TOP // (4 * EPD * mesh.shape["ep"])
        rows = EPD * S * SL
        sem = pltpu.SemaphoreType.DMA
        y = pl.pallas_call(
            functools.partial(kernel, S, EPD, TOP),
            out_shape=jax.ShapeDtypeStruct((T, D), x.dtype),
            in_specs=[pl.BlockSpec(memory_space=pl.ANY)]
            + [pl.BlockSpec(memory_space=pltpu.VMEM)] * 3
            + [pl.BlockSpec(memory_space=pl.ANY)] * 6,
            out_specs=pl.BlockSpec(memory_space=pltpu.VMEM),
            scratch_shapes=[
                pltpu.VMEM((T, D), BF16),
                pltpu.VMEM((16, T), F32),
                pltpu.VMEM((2, T, 128), F32),
                pltpu.VMEM((2, S - 1, T, H), BF16),
                pltpu.VMEM((2, S, 16, T), F32),
                pltpu.VMEM((2, rows, T), BF16),
                pltpu.VMEM((2, S - 1, rows, H), BF16),
                pltpu.VMEM((2, EPD, S, S * SL, H), BF16),
                pltpu.VMEM((S * S * SL, D), BF16),
                pltpu.VMEM((2, EPD, S, S * SL, H), BF16),
                pltpu.VMEM((2, 2, T // 2, H), BF16),
                pltpu.VMEM((2, 2, T, H), BF16),
                pltpu.VMEM((2, S, T, 2 * EPD * S * LO), BF16),
                pltpu.VMEM((S * S * SL, FF), BF16),
                pltpu.VMEM((T, D), F32),
                pltpu.VMEM((2, 2, D, CT), BF16),
                pltpu.VMEM((DB, FF, CT), BF16),
                sem, sem((2, 2)), sem((DB,)),
                sem((2, 6)), sem((2, 6)),
                sem((2, S - 1)), sem((2, S - 1)),
                sem((2, EPD, S - 1, 2)), sem((2, EPD, S - 1, 2)),
                sem((2, EPD, S - 1, 2)), sem((2, EPD, S - 1, 2)),
                sem((2, 2)), sem((2, 2)),
                sem((2, 2, 2)), sem((2, 2, 2)),
            ],
            compiler_params=pltpu.CompilerParams(
                collective_id=0, has_side_effects=True, vmem_limit_bytes=67043328
            ),
        )(x.reshape(T, D), *(v.reshape(T, TOP) for v in (expert, slot, gate)), w_gate, w_up, w_down, s_gate, s_up, s_down)
        return y.reshape(x.shape)

    own, experts, whole = P("dp", "ep"), P("ep"), P()
    return jax.shard_map(
        local,
        mesh=mesh,
        in_specs=(own,) * 4 + (experts,) * 3 + (whole,) * 3,
        out_specs=own,
        check_vma=False,
    )
```

```python
import functools
import math

import jax
import jax.numpy as jnp
from jax import lax
from jax.experimental import pallas as pl
from jax.experimental.pallas import tpu as pltpu
from jax.sharding import PartitionSpec as P

F32, BF16 = jnp.float32, jnp.bfloat16
LO, HI = 16, 8
CT = 256
DB = 4
EARLY = 1


def dot(a, b):
    return jnp.dot(a, b, preferred_element_type=F32)


def cols(i):
    return pl.ds(pl.multiple_of(i * CT, CT), CT)


def kernel(
    S, EPD, TOP,
    x_hbm, expert_ref, slot_ref, gate_ref, wg, wu, wd, sg, su, sd, y_ref,
    x_ref, meta_ref, ag, mall, oh, dsend, z, zf, crecv, via, fin, cmat, h, ysh, gu, db,
    x_sem, gu_sem, db_sem, ag_s, ag_r, m_s, m_r, z_s, z_r, c_s, c_r, v_s, v_r, f_s, f_r,
):
    T, D = x_ref.shape
    FF = wg.shape[2]
    H = D // 2
    SL = LO + HI
    CH = S * SL
    HT = T // 2
    PR = 2 * SL
    LAST = EPD + 1
    NG, NDT = FF // CT, D // CT
    HTILES = H // CT
    me = lax.axis_index("ep")
    px, py = lax.div(me, S), lax.rem(me, S)

    def dev(p, df, ds):
        dx = df * (1 - p) + ds * p
        dy = df * p + ds * (1 - p)
        return lax.rem(px + dx, S) * S + lax.rem(py + dy, S)

    def lo(r):
        return (r // 2) * PR + (r % 2) * LO

    def hi(r):
        return (r // 2) * PR + 2 * LO + (r % 2) * HI

    def start_gu(n):
        slot = lax.rem(n, 2)
        u, c = lax.div(n, NG), lax.rem(n, NG)

        @pl.when(jnp.logical_or(u == 0, u == LAST))
        def _():
            at = cols(c + lax.div(u, LAST) * NG)
            pltpu.make_async_copy(sg.at[:, at], gu.at[slot, 0], gu_sem.at[slot, 0]).start()
            pltpu.make_async_copy(su.at[:, at], gu.at[slot, 1], gu_sem.at[slot, 1]).start()

        @pl.when(jnp.logical_and(u > 0, u < LAST))
        def _():
            pltpu.make_async_copy(wg.at[u - 1, :, cols(c)], gu.at[slot, 0], gu_sem.at[slot, 0]).start()
            pltpu.make_async_copy(wu.at[u - 1, :, cols(c)], gu.at[slot, 1], gu_sem.at[slot, 1]).start()

    def wait_gu(n):
        slot = lax.rem(n, 2)
        for j in range(2):
            pltpu.make_async_copy(sg.at[:, cols(0)], gu.at[slot, j], gu_sem.at[slot, j]).wait()
        return slot

    def start_db(m):
        slot = lax.rem(m, DB)
        u, c = lax.div(m, NDT), lax.rem(m, NDT)

        @pl.when(jnp.logical_or(u == 0, u == LAST))
        def _():
            rows = pl.ds(pl.multiple_of(lax.div(u, LAST) * FF, FF), FF)
            pltpu.make_async_copy(sd.at[rows, cols(c)], db.at[slot], db_sem.at[slot]).start()

        @pl.when(jnp.logical_and(u > 0, u < LAST))
        def _():
            pltpu.make_async_copy(wd.at[u - 1, :, cols(c)], db.at[slot], db_sem.at[slot]).start()

    def wait_db(m):
        slot = lax.rem(m, DB)
        pltpu.make_async_copy(wd.at[0, :, cols(0)], db.at[slot], db_sem.at[slot]).wait()
        return slot

    x_copy = pltpu.make_async_copy(x_hbm, x_ref, x_sem)
    x_copy.start()
    start_gu(jnp.int32(0))
    for m in range(DB - 1):
        start_db(jnp.int32(m))

    barrier = pltpu.get_barrier_semaphore()
    for p in range(2):
        for d in range(1, S):
            pl.semaphore_signal(barrier, inc=1, device_id={"ep": dev(p, d, 0)})
    pl.semaphore_wait(barrier, 2 * (S - 1))

    def remote(src, dst, s, r, to):
        return pltpu.make_async_remote_copy(src, dst, s, r, device_id={"ep": to})

    def ag_first(p, d, early):
        i = 0 if d == 1 else 1
        rows = pl.ds((i if early else 1 - i) * HT, HT)
        n = i if early else 2 + i
        return remote(
            x_hbm.at[rows, pl.ds(p * H, H)], ag.at[p, S - d - 1, rows],
            ag_s.at[p, n], ag_r.at[p, n], dev(p, d, 0),
        )

    def ag_relay(p, d):
        i = 0 if d == 1 else 1
        rows = pl.ds(i * HT, HT)
        src = ag.at[p, (S - 1 if d == 1 else 1) - 1, rows]
        return remote(src, ag.at[p, 1, rows], ag_s.at[p, 4 + i], ag_r.at[p, 4 + i], dev(p, d, 0))

    def meta_copy(p, d):
        return remote(meta_ref, mall.at[p, S - d], m_s.at[p, d - 1], m_r.at[p, S - d - 1], dev(p, d, 0))

    for early in (True, False):
        for p in range(2):
            for d in (1, S - 1):
                ag_first(p, d, early).start()

    meta_ref[...] = jnp.zeros(meta_ref.shape, F32)
    for j in range(TOP):
        slot = slot_ref[j]
        meta_ref[j : j + 1] = jnp.where(slot < SL, expert_ref[j] * SL + slot, -1).astype(F32)
        meta_ref[8 + j : 9 + j] = gate_ref[j]
    for p in range(2):
        mall[p, 0] = meta_ref[...]
        for d in range(1, S):
            meta_copy(p, d).start()

    def up(lhs, rows, u):
        def tile(i, _):
            n = u * NG + i
            slot = wait_gu(n)
            pl.when(n + 1 < (LAST + 1) * NG)(lambda: start_gu(n + 1))
            g = dot(lhs[...], gu[slot, 0])
            v = dot(lhs[...], gu[slot, 1])
            h[0:rows, cols(i)] = (jax.nn.silu(g) * v).astype(BF16)
            return 0

        lax.fori_loop(0, NG, tile, 0)

    def down_tile(rows, u, c):
        m = u * NDT + c
        slot = wait_db(m)
        pl.when(m + DB - 1 < (LAST + 1) * NDT)(lambda: start_db(m + DB - 1))
        return dot(h[0:rows, :], db[slot])

    def shared_down(u):
        def tile(c, _):
            o = down_tile(T, u, c)
            ysh[:, cols(c)] = o if u == 0 else ysh[:, cols(c)] + o
            return 0

        lax.fori_loop(0, NDT, tile, 0)

    x_copy.wait()
    up(x_ref, T, 0)
    for p in range(2):
        for d in (1, S - 1):
            ag_first(p, d, True).wait_recv()
        ag_relay(p, 1).start()
        ag_relay(p, S - 1).start()
    shared_down(0)

    for p in range(2):
        for d in (1, S - 1):
            ag_first(p, d, False).wait_recv()
        for d in range(1, S):
            meta_copy(p, d).wait_recv()

    def source(p, r, c):
        if r == 0:
            return x_ref[:, pl.ds(pl.multiple_of(p * H + c * CT, CT), CT)]
        return ag[p, r - 1, :, cols(c)]

    def onehot(p, r):
        i = lax.broadcasted_iota(jnp.int32, (S * EPD * SL, T), 0)
        n = EPD * SL
        off = dev(p, 0, S - 1) * n - (S - 1) * n
        for k in range(S - 2, -1, -1):
            off = jnp.where(i < (k + 1) * n, (dev(p, 0, k) - k) * n, off)
        code = (i + off).astype(F32)
        total = jnp.zeros(code.shape, F32)
        for j in range(TOP):
            total += jnp.where(code == mall[p, r, j : j + 1, :], 1.0, 0.0)
        return total.astype(BF16)

    def select(p, pair):
        for j in range(2):
            oh[j] = onehot(p, 2 * pair + j)

        def tile(c, _):
            a = dot(oh[0], source(p, 2 * pair, c))
            b = dot(oh[1], source(p, 2 * pair + 1, c))
            for k in range(S):
                for e in range(EPD):
                    o = (k * EPD + e) * SL
                    m = o + LO
                    b48 = jnp.concatenate([a[o:m], b[o:m], a[m : o + SL], b[m : o + SL]], 0)
                    at = pair * PR
                    if k == 0:
                        z[p, e, 0, at : at + PR, cols(c)] = b48.astype(BF16)
                    else:
                        at += e * CH
                        dsend[p, k - 1, at : at + PR, cols(c)] = b48.astype(BF16)
            return 0

        lax.fori_loop(0, HTILES, tile, 0)

    def halves(e):
        return (0, 1) if e < EARLY else (2,)

    def z_copy(p, e, k, half):
        at, n = (half * PR, PR) if half < 2 else (0, CH)
        rows = pl.ds(pl.multiple_of(e * CH + at, PR), n)
        return remote(
            dsend.at[p, k - 1, rows], z.at[p, e, S - k, pl.ds(at, n)],
            z_s.at[p, e, k - 1, half % 2], z_r.at[p, e, S - k - 1, half % 2], dev(p, 0, k),
        )

    def z_start(e, half):
        for k in (1, S - 1, 2):
            for p in range(2):
                z_copy(p, e, k, half).start()

    for p in range(2):
        select(p, 0)
    for e in range(EARLY):
        z_start(e, 0)
    for p in range(2):
        for d in (1, S - 1):
            ag_relay(p, d).wait_recv()
    for p in range(2):
        select(p, 1)
    for e in range(EPD):
        z_start(e, 1 if e < EARLY else 2)

    def coefficients(n, _):
        p, r = lax.div(n, S), lax.rem(n, S)
        half = EPD * S * LO
        i = lax.broadcasted_iota(jnp.int32, (2 * half, T), 0)
        high = i >= half
        i = jnp.where(high, i - half, i)
        e, kk, c = i >> 6, (i >> 4) & 3, i & 15
        owner = jnp.where(kk == 0, dev(p, 0, 0), 0)
        for k in range(1, S):
            owner = jnp.where(kk == k, dev(p, 0, k), owner)
        odd = c >> 3
        slot = jnp.where(high, LO + (c & 7), c)
        code = (owner * EPD + e) * SL + slot
        code = jnp.where(jnp.logical_and(high, odd != lax.rem(r, 2)), -2, code).astype(F32)
        total = jnp.zeros(code.shape, F32)
        for j in range(TOP):
            total += jnp.where(code == mall[p, r, j : j + 1, :], mall[p, r, 8 + j : 9 + j, :], 0.0)
        cmat[p, r] = total.T.astype(BF16)
        return 0

    lax.fori_loop(0, 2 * S, coefficients, 0)

    def c_copy(p, e, k, half):
        at, n = (half * PR, PR) if half < 2 else (0, CH)
        return remote(
            z.at[p, e, k, pl.ds(at, n)], crecv.at[p, e, S - k, pl.ds(at, n)],
            c_s.at[p, e, k - 1, half % 2], c_r.at[p, e, S - k - 1, half % 2], dev(p, 0, k),
        )

    def expert(e, _):
        def arrived(half):
            for k in (1, S - 1, 2):
                for p in range(2):
                    z_copy(p, e, k, half).wait_recv()

        @pl.when(e < EARLY)
        def _():
            arrived(0)
            arrived(1)

        @pl.when(e >= EARLY)
        def _():
            arrived(2)

        for k in range(S):
            zf[k * CH : (k + 1) * CH, 0:H] = z[0, e, k]
            for r in range(S):
                o = k * CH + lo(r)
                zf[o : o + LO, H:D] = z[1, e, r, lo(k) : lo(k) + LO]
            u0 = hi(k) - (k % 2) * HI
            for r in range(0, S, 2):
                o = k * CH + hi(r)
                two = [
                    z[1, e, r + j, u0 : u0 + 2 * HI].astype(F32)[(k % 2) * HI : (k % 2 + 1) * HI]
                    for j in range(2)
                ]
                zf[o : o + 2 * HI, H:D] = jnp.concatenate(two, 0).astype(BF16)

        up(zf, S * CH, 1 + e)

        def back(p, half):
            for k in (1, S - 1, 2):
                c_copy(p, e, k, half).start()

        for p in range(2):

            def tile(c, _):
                o = down_tile(S * CH, 1 + e, p * HTILES + c)
                for k in range(S):
                    if p == 0:
                        b = o[k * CH : (k + 1) * CH]
                    else:
                        rows = []
                        for r in range(0, S, 2):
                            for f, n in ((lo(k), LO), (hi(k), HI)):
                                rows += [o[q * CH + f : q * CH + f + n] for q in (r, r + 1)]
                        b = jnp.concatenate(rows, 0)
                    if k == 0:
                        crecv[p, e, 0, :, cols(c)] = b.astype(BF16)
                    else:
                        z[p, e, k, :, cols(c)] = b.astype(BF16)
                return 0

            lax.fori_loop(0, HTILES, tile, 0)
            pl.when(e < EPD - 1)(lambda: back(p, 2))

        @pl.when(e == EPD - 1)
        def _():
            for half in (1, 0):
                for p in range(2):
                    back(p, half)

        return 0

    lax.fori_loop(0, EPD, expert, 0)
    up(x_ref, T, LAST)
    shared_down(LAST)

    for p in range(2):
        for e in range(EPD):
            for k in range(1, S):
                for half in halves(e):
                    z_copy(p, e, k, half).wait_send()

    def slots(p, r, c):
        a = crecv[p, :, :, lo(r) : lo(r) + LO, cols(c)].reshape(EPD * S * LO, CT)
        u0 = hi(r) - (r % 2) * HI
        b = crecv[p, :, :, u0 : u0 + 2 * HI, cols(c)].reshape(EPD * S * LO, CT)
        return jnp.concatenate([a, b], 0)

    def part(p, r, c, r0, r1):
        return dot(cmat[p, r, r0:r1], slots(p, r, c))

    def via_copy(p, i):
        src = dsend.at[p, 1, pl.ds(i * HT, HT)]
        return remote(src, via.at[p, i], v_s.at[p, i], v_r.at[p, i], dev(p, 1 if i == 0 else S - 1, 0))

    def fin_copy(p, i, half):
        src = dsend.at[p, 2 * i, pl.ds(half * HT, HT)]
        dst = fin.at[p, i, pl.ds(half * HT, HT)]
        return remote(src, dst, f_s.at[p, i, half], f_r.at[p, i, half], dev(p, 1 if i == 0 else S - 1, 0))

    for p in range(2):
        for e in range(EPD):
            for k in range(1, S):
                c_copy(p, e, k, 2 if e < EPD - 1 else 1).wait_recv()

        def far(c, _):
            dsend[p, 1, 0:T, cols(c)] = part(p, 2, c, 0, T).astype(BF16)
            return 0

        lax.fori_loop(0, HTILES, far, 0)
        for i in range(2):
            via_copy(p, i).start()

    for p in range(2):

        def before(c, _):
            dsend[p, 2, 0:HT, cols(c)] = part(p, S - 1, c, 0, HT).astype(BF16)
            return 0

        lax.fori_loop(0, HTILES, before, 0)
        fin_copy(p, 1, 0).start()

    for p in range(2):
        for k in range(1, S):
            c_copy(p, EPD - 1, k, 0).wait_recv()

        def after(c, _):
            dsend[p, 0, HT:T, cols(c)] = part(p, 1, c, HT, T).astype(BF16)
            return 0

        lax.fori_loop(0, HTILES, after, 0)
        fin_copy(p, 0, 1).start()

    for p in range(2):
        for i in range(2):
            via_copy(p, i).wait_recv()

        def through(c, _):
            a = part(p, 1, c, 0, HT) + via[p, 0, :, cols(c)].astype(F32)
            b = part(p, S - 1, c, HT, T) + via[p, 1, :, cols(c)].astype(F32)
            dsend[p, 0, 0:HT, cols(c)] = a.astype(BF16)
            dsend[p, 2, HT:T, cols(c)] = b.astype(BF16)
            return 0

        lax.fori_loop(0, HTILES, through, 0)
        fin_copy(p, 0, 0).start()
        fin_copy(p, 1, 1).start()

    for p in range(2):

        def own(c, _):
            ysh[:, cols(p * HTILES + c)] += part(p, 0, c, 0, T)
            return 0

        lax.fori_loop(0, HTILES, own, 0)

    for p in range(2):
        for i in range(2):
            for half in range(2):
                fin_copy(p, i, half).wait_recv()

        def last(c, _):
            a = fin[p, 0, :, cols(c)].astype(F32) + fin[p, 1, :, cols(c)].astype(F32)
            at = cols(p * HTILES + c)
            y_ref[:, at] = (ysh[:, at] + a).astype(y_ref.dtype)
            return 0

        lax.fori_loop(0, HTILES, last, 0)

    for p in range(2):
        for d in range(1, S):
            meta_copy(p, d).wait_send()
        for d in (1, S - 1):
            for early in (True, False):
                ag_first(p, d, early).wait_send()
            ag_relay(p, d).wait_send()
        for e in range(EPD):
            for k in range(1, S):
                for half in (2,) if e < EPD - 1 else (0, 1):
                    c_copy(p, e, k, half).wait_send()
        for i in range(2):
            via_copy(p, i).wait_send()
            for half in range(2):
                fin_copy(p, i, half).wait_send()


def solution(mesh):
    side = math.isqrt(mesh.shape["ep"])

    def local(x, expert, slot, gate, w_gate, w_up, w_down, s_gate, s_up, s_down):
        T, D = x.shape[2:]
        TOP = expert.shape[3]
        EPD, _, FF = w_gate.shape
        SL, S, H = LO + HI, side, D // 2
        assert side * side == mesh.shape["ep"] and side == 4
        assert FF * 2 == s_gate.shape[1] and SL == 5 * T * TOP // (4 * EPD * mesh.shape["ep"])
        rows = EPD * S * SL
        sem = pltpu.SemaphoreType.DMA
        y = pl.pallas_call(
            functools.partial(kernel, S, EPD, TOP),
            out_shape=jax.ShapeDtypeStruct((T, D), x.dtype),
            in_specs=[pl.BlockSpec(memory_space=pl.ANY)]
            + [pl.BlockSpec(memory_space=pltpu.VMEM)] * 3
            + [pl.BlockSpec(memory_space=pl.ANY)] * 6,
            out_specs=pl.BlockSpec(memory_space=pltpu.VMEM),
            scratch_shapes=[
                pltpu.VMEM((T, D), BF16),
                pltpu.VMEM((16, T), F32),
                pltpu.VMEM((2, S - 1, T, H), BF16),
                pltpu.VMEM((2, S, 16, T), F32),
                pltpu.VMEM((2, rows, T), BF16),
                pltpu.VMEM((2, S - 1, rows, H), BF16),
                pltpu.VMEM((2, EPD, S, S * SL, H), BF16),
                pltpu.VMEM((S * S * SL, D), BF16),
                pltpu.VMEM((2, EPD, S, S * SL, H), BF16),
                pltpu.VMEM((2, 2, T // 2, H), BF16),
                pltpu.VMEM((2, 2, T, H), BF16),
                pltpu.VMEM((2, S, T, 2 * EPD * S * LO), BF16),
                pltpu.VMEM((S * S * SL, FF), BF16),
                pltpu.VMEM((T, D), F32),
                pltpu.VMEM((2, 2, D, CT), BF16),
                pltpu.VMEM((DB, FF, CT), BF16),
                sem, sem((2, 2)), sem((DB,)),
                sem((2, 6)), sem((2, 6)),
                sem((2, S - 1)), sem((2, S - 1)),
                sem((2, EPD, S - 1, 2)), sem((2, EPD, S - 1, 2)),
                sem((2, EPD, S - 1, 2)), sem((2, EPD, S - 1, 2)),
                sem((2, 2)), sem((2, 2)),
                sem((2, 2, 2)), sem((2, 2, 2)),
            ],
            compiler_params=pltpu.CompilerParams(
                collective_id=0, has_side_effects=True, vmem_limit_bytes=67043328
            ),
        )(x.reshape(T, D), *(v.transpose(0, 3, 1, 2).reshape(TOP, 1, T) for v in (expert, slot, gate)), w_gate, w_up, w_down, s_gate, s_up, s_down)
        return y.reshape(x.shape)

    own, experts, whole = P("dp", "ep"), P("ep"), P()
    return jax.shard_map(
        local,
        mesh=mesh,
        in_specs=(own,) * 4 + (experts,) * 3 + (whole,) * 3,
        out_specs=own,
        check_vma=False,
    )
```

```python
import functools
import math

import jax
import jax.numpy as jnp
from jax import lax
from jax.experimental import pallas as pl
from jax.experimental.pallas import tpu as pltpu
from jax.sharding import PartitionSpec as P

F32, BF16 = jnp.float32, jnp.bfloat16
LO, HI = 16, 8
CT = 256
DB = 4
GB = 3
EARLY = 1


def dot(a, b):
    return jnp.dot(a, b, preferred_element_type=F32)


def cols(i):
    return pl.ds(pl.multiple_of(i * CT, CT), CT)


def kernel(
    S, EPD, TOP,
    x_hbm, expert_hbm, slot_hbm, gate_hbm, wg, wu, wd, sg, su, sd, sum_ref, late_ref,
    x_ref, expert_ref, slot_ref, gate_ref, meta_ref, ag, mall, oh, dsend, z, zf, crecv, via, fin, cmat, h, ysh, gu, db,
    x_sem, i_sem, y_sem, gu_sem, db_sem, ag_s, ag_r, m_s, m_r, z_s, z_r, c_s, c_r, v_s, v_r, f_s, f_r,
):
    T, D = x_ref.shape
    FF = wg.shape[2]
    H = D // 2
    SL = LO + HI
    CH = S * SL
    HT = T // 2
    PR = 2 * SL
    LAST = EPD + 1
    NG, NDT = FF // CT, D // CT
    HTILES = H // CT
    me = lax.axis_index("ep")
    px, py = lax.div(me, S), lax.rem(me, S)

    def dev(p, df, ds):
        dx = df * (1 - p) + ds * p
        dy = df * p + ds * (1 - p)
        return lax.rem(px + dx, S) * S + lax.rem(py + dy, S)

    def lo(r):
        return (r // 2) * PR + (r % 2) * LO

    def hi(r):
        return (r // 2) * PR + 2 * LO + (r % 2) * HI

    def start_gu(n):
        slot = lax.rem(n, GB)
        u, c = lax.div(n, NG), lax.rem(n, NG)

        @pl.when(jnp.logical_or(u == 0, u == LAST))
        def _():
            at = cols(c + lax.div(u, LAST) * NG)
            pltpu.make_async_copy(sg.at[:, at], gu.at[slot, 0], gu_sem.at[slot, 0]).start()
            pltpu.make_async_copy(su.at[:, at], gu.at[slot, 1], gu_sem.at[slot, 1]).start()

        @pl.when(jnp.logical_and(u > 0, u < LAST))
        def _():
            pltpu.make_async_copy(wg.at[u - 1, :, cols(c)], gu.at[slot, 0], gu_sem.at[slot, 0]).start()
            pltpu.make_async_copy(wu.at[u - 1, :, cols(c)], gu.at[slot, 1], gu_sem.at[slot, 1]).start()

    def wait_gu(n):
        slot = lax.rem(n, GB)
        for j in range(2):
            pltpu.make_async_copy(sg.at[:, cols(0)], gu.at[slot, j], gu_sem.at[slot, j]).wait()
        return slot

    def start_db(m):
        slot = lax.rem(m, DB)
        u, c = lax.div(m, NDT), lax.rem(m, NDT)

        @pl.when(jnp.logical_or(u == 0, u == LAST))
        def _():
            rows = pl.ds(pl.multiple_of(lax.div(u, LAST) * FF, FF), FF)
            pltpu.make_async_copy(sd.at[rows, cols(c)], db.at[slot], db_sem.at[slot]).start()

        @pl.when(jnp.logical_and(u > 0, u < LAST))
        def _():
            pltpu.make_async_copy(wd.at[u - 1, :, cols(c)], db.at[slot], db_sem.at[slot]).start()

    def wait_db(m):
        slot = lax.rem(m, DB)
        pltpu.make_async_copy(wd.at[0, :, cols(0)], db.at[slot], db_sem.at[slot]).wait()
        return slot

    x_copy = pltpu.make_async_copy(x_hbm, x_ref, x_sem)
    routing = [
        pltpu.make_async_copy(a, b, i_sem.at[i])
        for i, (a, b) in enumerate(
            ((expert_hbm, expert_ref), (slot_hbm, slot_ref), (gate_hbm, gate_ref))
        )
    ]
    barrier = pltpu.get_barrier_semaphore()
    for p in range(2):
        for d in range(1, S):
            pl.semaphore_signal(barrier, inc=1, device_id={"ep": dev(p, d, 0)})
    for copy in routing:
        copy.start()
    x_copy.start()
    for n in range(GB - 1):
        start_gu(jnp.int32(n))
    for m in range(DB - 1):
        start_db(jnp.int32(m))
    pl.semaphore_wait(barrier, 2 * (S - 1))

    def remote(src, dst, s, r, to):
        return pltpu.make_async_remote_copy(src, dst, s, r, device_id={"ep": to})

    def ag_first(p, d, early):
        i = 0 if d == 1 else 1
        rows = pl.ds((i if early else 1 - i) * HT, HT)
        n = i if early else 2 + i
        return remote(
            x_hbm.at[rows, pl.ds(p * H, H)], ag.at[p, S - d - 1, rows],
            ag_s.at[p, n], ag_r.at[p, n], dev(p, d, 0),
        )

    def ag_relay(p, d):
        i = 0 if d == 1 else 1
        rows = pl.ds(i * HT, HT)
        src = ag.at[p, (S - 1 if d == 1 else 1) - 1, rows]
        return remote(src, ag.at[p, 1, rows], ag_s.at[p, 4 + i], ag_r.at[p, 4 + i], dev(p, d, 0))

    def meta_copy(p, d):
        return remote(meta_ref, mall.at[p, S - d], m_s.at[p, d - 1], m_r.at[p, S - d - 1], dev(p, d, 0))

    for early in (True, False):
        for p in range(2):
            for d in (1, S - 1):
                ag_first(p, d, early).start()

    for copy in routing:
        copy.wait()
    meta_ref[...] = jnp.zeros(meta_ref.shape, F32)
    for j in range(TOP):
        slot = slot_ref[j]
        meta_ref[j : j + 1] = jnp.where(slot < SL, expert_ref[j] * SL + slot, -1).astype(F32)
        meta_ref[8 + j : 9 + j] = gate_ref[j]
    for p in range(2):
        mall[p, 0] = meta_ref[...]
        for d in range(1, S):
            meta_copy(p, d).start()

    def up(lhs, rows, u):
        def tile(i, _):
            n = u * NG + i
            slot = wait_gu(n)
            pl.when(n + GB - 1 < (LAST + 1) * NG)(lambda: start_gu(n + GB - 1))
            g = dot(lhs[...], gu[slot, 0])
            v = dot(lhs[...], gu[slot, 1])
            h[0:rows, cols(i)] = (jax.nn.silu(g) * v).astype(BF16)
            return 0

        lax.fori_loop(0, NG, tile, 0)

    def down_tile(rows, u, c):
        m = u * NDT + c
        slot = wait_db(m)
        pl.when(m + DB - 1 < (LAST + 1) * NDT)(lambda: start_db(m + DB - 1))
        return dot(h[0:rows, :], db[slot])

    def shared_down(u):
        def tile(c, _):
            o = down_tile(T, u, c)
            ysh[:, cols(c)] = o if u == 0 else ysh[:, cols(c)] + o
            return 0

        lax.fori_loop(0, NDT, tile, 0)

    x_copy.wait()
    up(x_ref, T, 0)
    for p in range(2):
        for d in (1, S - 1):
            ag_first(p, d, True).wait_recv()
        ag_relay(p, 1).start()
        ag_relay(p, S - 1).start()
    shared_down(0)

    for p in range(2):
        for d in (1, S - 1):
            ag_first(p, d, False).wait_recv()
        for d in range(1, S):
            meta_copy(p, d).wait_recv()

    def source(p, r, c):
        if r == 0:
            return x_ref[:, pl.ds(pl.multiple_of(p * H + c * CT, CT), CT)]
        return ag[p, r - 1, :, cols(c)]

    def onehot(p, r):
        i = lax.broadcasted_iota(jnp.int32, (S * EPD * SL, T), 0)
        n = EPD * SL
        off = dev(p, 0, S - 1) * n - (S - 1) * n
        for k in range(S - 2, -1, -1):
            off = jnp.where(i < (k + 1) * n, (dev(p, 0, k) - k) * n, off)
        code = (i + off).astype(F32)
        total = jnp.zeros(code.shape, F32)
        for j in range(TOP):
            total += jnp.where(code == mall[p, r, j : j + 1, :], 1.0, 0.0)
        return total.astype(BF16)

    def select(p, pair):
        for j in range(2):
            oh[j] = onehot(p, 2 * pair + j)

        def tile(c, _):
            a = dot(oh[0], source(p, 2 * pair, c))
            b = dot(oh[1], source(p, 2 * pair + 1, c))
            for k in range(S):
                for e in range(EPD):
                    o = (k * EPD + e) * SL
                    m = o + LO
                    b48 = jnp.concatenate([a[o:m], b[o:m], a[m : o + SL], b[m : o + SL]], 0)
                    at = pair * PR
                    if k == 0:
                        z[p, e, 0, at : at + PR, cols(c)] = b48.astype(BF16)
                    else:
                        at += e * CH
                        dsend[p, k - 1, at : at + PR, cols(c)] = b48.astype(BF16)
            return 0

        lax.fori_loop(0, HTILES, tile, 0)

    def halves(e):
        return (0, 1) if e < EARLY else (2,)

    def z_copy(p, e, k, half):
        at, n = (half * PR, PR) if half < 2 else (0, CH)
        rows = pl.ds(pl.multiple_of(e * CH + at, PR), n)
        return remote(
            dsend.at[p, k - 1, rows], z.at[p, e, S - k, pl.ds(at, n)],
            z_s.at[p, e, k - 1, half % 2], z_r.at[p, e, S - k - 1, half % 2], dev(p, 0, k),
        )

    def z_start(e, half):
        for k in (1, S - 1, 2):
            for p in range(2):
                z_copy(p, e, k, half).start()

    for p in range(2):
        select(p, 0)
    for e in range(EARLY):
        z_start(e, 0)
    for p in range(2):
        for d in (1, S - 1):
            ag_relay(p, d).wait_recv()
    for p in range(2):
        select(p, 1)
    for e in range(EPD):
        z_start(e, 1 if e < EARLY else 2)

    def coefficients(n, _):
        p, r = lax.div(n, S), lax.rem(n, S)
        half = EPD * S * LO
        i = lax.broadcasted_iota(jnp.int32, (2 * half, T), 0)
        high = i >= half
        i = jnp.where(high, i - half, i)
        e, kk, c = i >> 6, (i >> 4) & 3, i & 15
        owner = jnp.where(kk == 0, dev(p, 0, 0), 0)
        for k in range(1, S):
            owner = jnp.where(kk == k, dev(p, 0, k), owner)
        odd = c >> 3
        slot = jnp.where(high, LO + (c & 7), c)
        code = (owner * EPD + e) * SL + slot
        code = jnp.where(jnp.logical_and(high, odd != lax.rem(r, 2)), -2, code).astype(F32)
        total = jnp.zeros(code.shape, F32)
        for j in range(TOP):
            total += jnp.where(code == mall[p, r, j : j + 1, :], mall[p, r, 8 + j : 9 + j, :], 0.0)
        cmat[p, r] = total.T.astype(BF16)
        return 0

    lax.fori_loop(0, 2 * S, coefficients, 0)

    def c_copy(p, e, k, half):
        at, n = (half * PR, PR) if half < 2 else (0, CH)
        return remote(
            z.at[p, e, k, pl.ds(at, n)], crecv.at[p, e, S - k, pl.ds(at, n)],
            c_s.at[p, e, k - 1, half % 2], c_r.at[p, e, S - k - 1, half % 2], dev(p, 0, k),
        )

    def expert(e, _):
        def arrived(half):
            for k in (1, S - 1, 2):
                for p in range(2):
                    z_copy(p, e, k, half).wait_recv()

        @pl.when(e < EARLY)
        def _():
            arrived(0)
            arrived(1)

        @pl.when(e >= EARLY)
        def _():
            arrived(2)

        for k in range(S):
            zf[k * CH : (k + 1) * CH, 0:H] = z[0, e, k]
            for r in range(S):
                o = k * CH + lo(r)
                zf[o : o + LO, H:D] = z[1, e, r, lo(k) : lo(k) + LO]
            u0 = hi(k) - (k % 2) * HI
            for r in range(0, S, 2):
                o = k * CH + hi(r)
                two = [
                    z[1, e, r + j, u0 : u0 + 2 * HI].astype(F32)[(k % 2) * HI : (k % 2 + 1) * HI]
                    for j in range(2)
                ]
                zf[o : o + 2 * HI, H:D] = jnp.concatenate(two, 0).astype(BF16)

        up(zf, S * CH, 1 + e)

        def back(p, half):
            for k in (1, S - 1, 2):
                c_copy(p, e, k, half).start()

        for p in range(2):

            def tile(c, _):
                o = down_tile(S * CH, 1 + e, p * HTILES + c)
                for k in range(S):
                    if p == 0:
                        b = o[k * CH : (k + 1) * CH]
                    else:
                        rows = []
                        for r in range(0, S, 2):
                            for f, n in ((lo(k), LO), (hi(k), HI)):
                                rows += [o[q * CH + f : q * CH + f + n] for q in (r, r + 1)]
                        b = jnp.concatenate(rows, 0)
                    if k == 0:
                        crecv[p, e, 0, :, cols(c)] = b.astype(BF16)
                    else:
                        z[p, e, k, :, cols(c)] = b.astype(BF16)
                return 0

            lax.fori_loop(0, HTILES, tile, 0)
            pl.when(e < EPD - 1)(lambda: back(p, 2))

        @pl.when(e == EPD - 1)
        def _():
            for half in (1, 0):
                for p in range(2):
                    back(p, half)

        return 0

    lax.fori_loop(0, EPD, expert, 0)
    up(x_ref, T, LAST)
    shared_down(LAST)

    for p in range(2):
        for e in range(EPD):
            for k in range(1, S):
                for half in halves(e):
                    z_copy(p, e, k, half).wait_send()

    def slots(p, r, c):
        a = crecv[p, :, :, lo(r) : lo(r) + LO, cols(c)].reshape(EPD * S * LO, CT)
        u0 = hi(r) - (r % 2) * HI
        b = crecv[p, :, :, u0 : u0 + 2 * HI, cols(c)].reshape(EPD * S * LO, CT)
        return jnp.concatenate([a, b], 0)

    def part(p, r, c, r0, r1):
        return dot(cmat[p, r, r0:r1], slots(p, r, c))

    def via_copy(p, i):
        src = dsend.at[p, 1, pl.ds(i * HT, HT)]
        return remote(src, via.at[p, i], v_s.at[p, i], v_r.at[p, i], dev(p, 1 if i == 0 else S - 1, 0))

    def fin_copy(p, i, half):
        src = dsend.at[p, 2 * i, pl.ds(half * HT, HT)]
        if half == i:
            dst = late_ref.at[pl.ds(half * HT, HT), pl.ds(p * H, H)]
        else:
            dst = fin.at[p, i]
        return remote(src, dst, f_s.at[p, i, half], f_r.at[p, i, half], dev(p, 1 if i == 0 else S - 1, 0))

    for p in range(2):
        for e in range(EPD):
            for k in range(1, S):
                c_copy(p, e, k, 2 if e < EPD - 1 else 1).wait_recv()

        def far(c, _):
            dsend[p, 1, 0:T, cols(c)] = part(p, 2, c, 0, T).astype(BF16)
            return 0

        lax.fori_loop(0, HTILES, far, 0)
        for i in range(2):
            via_copy(p, i).start()

    for p in range(2):

        def before(c, _):
            dsend[p, 2, 0:HT, cols(c)] = part(p, S - 1, c, 0, HT).astype(BF16)
            return 0

        lax.fori_loop(0, HTILES, before, 0)
        fin_copy(p, 1, 0).start()

    for p in range(2):
        for k in range(1, S):
            c_copy(p, EPD - 1, k, 0).wait_recv()

        def after(c, _):
            dsend[p, 0, HT:T, cols(c)] = part(p, 1, c, HT, T).astype(BF16)
            return 0

        lax.fori_loop(0, HTILES, after, 0)
        fin_copy(p, 0, 1).start()

    for p in range(2):
        for i in range(2):
            via_copy(p, i).wait_recv()

        def through(c, _):
            a = part(p, 1, c, 0, HT) + via[p, 0, :, cols(c)].astype(F32)
            b = part(p, S - 1, c, HT, T) + via[p, 1, :, cols(c)].astype(F32)
            dsend[p, 0, 0:HT, cols(c)] = a.astype(BF16)
            dsend[p, 2, HT:T, cols(c)] = b.astype(BF16)
            return 0

        lax.fori_loop(0, HTILES, through, 0)
        fin_copy(p, 0, 0).start()
        fin_copy(p, 1, 1).start()

    for p in range(2):

        def own(c, _):
            ysh[:, cols(p * HTILES + c)] += part(p, 0, c, 0, T)
            return 0

        lax.fori_loop(0, HTILES, own, 0)

    def y_copy(p):
        half = pl.ds(p * H, H)
        return pltpu.make_async_copy(ysh.at[:, half], sum_ref.at[:, half], y_sem.at[p])

    for p in range(2):
        for i in range(2):
            fin_copy(p, i, 1 - i).wait_recv()

        def last(c, _):
            at = cols(p * HTILES + c)
            ysh[0:HT, at] += fin[p, 1, :, cols(c)].astype(F32)
            ysh[HT:T, at] += fin[p, 0, :, cols(c)].astype(F32)
            return 0

        lax.fori_loop(0, HTILES, last, 0)
        y_copy(p).start()
    for p in range(2):
        y_copy(p).wait()
        for i in range(2):
            fin_copy(p, i, i).wait_recv()

    for p in range(2):
        for d in range(1, S):
            meta_copy(p, d).wait_send()
        for d in (1, S - 1):
            for early in (True, False):
                ag_first(p, d, early).wait_send()
            ag_relay(p, d).wait_send()
        for e in range(EPD):
            for k in range(1, S):
                for half in (2,) if e < EPD - 1 else (0, 1):
                    c_copy(p, e, k, half).wait_send()
        for i in range(2):
            via_copy(p, i).wait_send()
            for half in range(2):
                fin_copy(p, i, half).wait_send()


def solution(mesh):
    side = math.isqrt(mesh.shape["ep"])

    def local(x, expert, slot, gate, w_gate, w_up, w_down, s_gate, s_up, s_down):
        T, D = x.shape[2:]
        TOP = expert.shape[3]
        EPD, _, FF = w_gate.shape
        SL, S, H = LO + HI, side, D // 2
        assert side * side == mesh.shape["ep"] and side == 4
        assert FF * 2 == s_gate.shape[1] and SL == 5 * T * TOP // (4 * EPD * mesh.shape["ep"])
        rows = EPD * S * SL
        sem = pltpu.SemaphoreType.DMA
        total, late = pl.pallas_call(
            functools.partial(kernel, S, EPD, TOP),
            out_shape=[jax.ShapeDtypeStruct((T, D), F32), jax.ShapeDtypeStruct((T, D), BF16)],
            in_specs=[pl.BlockSpec(memory_space=pl.ANY)] * 10,
            out_specs=[pl.BlockSpec(memory_space=pl.ANY)] * 2,
            scratch_shapes=[
                pltpu.VMEM((T, D), BF16),
                pltpu.VMEM((TOP, 1, T), jnp.int32),
                pltpu.VMEM((TOP, 1, T), jnp.int32),
                pltpu.VMEM((TOP, 1, T), F32),
                pltpu.VMEM((16, T), F32),
                pltpu.VMEM((2, S - 1, T, H), BF16),
                pltpu.VMEM((2, S, 16, T), F32),
                pltpu.VMEM((2, rows, T), BF16),
                pltpu.VMEM((2, S - 1, rows, H), BF16),
                pltpu.VMEM((2, EPD, S, S * SL, H), BF16),
                pltpu.VMEM((S * S * SL, D), BF16),
                pltpu.VMEM((2, EPD, S, S * SL, H), BF16),
                pltpu.VMEM((2, 2, T // 2, H), BF16),
                pltpu.VMEM((2, 2, T // 2, H), BF16),
                pltpu.VMEM((2, S, T, 2 * EPD * S * LO), BF16),
                pltpu.VMEM((S * S * SL, FF), BF16),
                pltpu.VMEM((T, D), F32),
                pltpu.VMEM((GB, 2, D, CT), BF16),
                pltpu.VMEM((DB, FF, CT), BF16),
                sem, sem((3,)), sem((2,)), sem((GB, 2)), sem((DB,)),
                sem((2, 6)), sem((2, 6)),
                sem((2, S - 1)), sem((2, S - 1)),
                sem((2, EPD, S - 1, 2)), sem((2, EPD, S - 1, 2)),
                sem((2, EPD, S - 1, 2)), sem((2, EPD, S - 1, 2)),
                sem((2, 2)), sem((2, 2)),
                sem((2, 2, 2)), sem((2, 2, 2)),
            ],
            compiler_params=pltpu.CompilerParams(
                collective_id=0, has_side_effects=True, vmem_limit_bytes=67043328
            ),
        )(x.reshape(T, D), *(v.transpose(0, 3, 1, 2).reshape(TOP, 1, T) for v in (expert, slot, gate)), w_gate, w_up, w_down, s_gate, s_up, s_down)
        return (total + late.astype(F32)).astype(x.dtype).reshape(x.shape)

    own, experts, whole = P("dp", "ep"), P("ep"), P()
    return jax.shard_map(
        local,
        mesh=mesh,
        in_specs=(own,) * 4 + (experts,) * 3 + (whole,) * 3,
        out_specs=own,
        check_vma=False,
    )
```

```python
import functools
import math

import jax
import jax.numpy as jnp
from jax import lax
from jax.experimental import pallas as pl
from jax.experimental.pallas import tpu as pltpu
from jax.sharding import PartitionSpec as P

F32, BF16 = jnp.float32, jnp.bfloat16
LO, HI = 16, 8
CT = 256
PARTS = 2
DB = 4
GB = 3
EARLY = 1


def dot(a, b):
    return jnp.dot(a, b, preferred_element_type=F32)


def cols(i):
    return pl.ds(pl.multiple_of(i * CT, CT), CT)


def kernel(
    S, EPD, TOP,
    x_hbm, expert_hbm, slot_hbm, gate_hbm, wg, wu, wd, sg, su, sd, sum_ref, late_ref,
    x_ref, expert_ref, slot_ref, gate_ref, meta_ref, ag, mall, oh, dsend, z, zf, crecv, via, fin, cmat, h, ysh, gu, db,
    x_sem, i_sem, y_sem, gu_sem, db_sem, ag_s, ag_r, m_s, m_r, z_s, z_r, c_s, c_r, v_s, v_r, f_s, f_r,
):
    T, D = x_ref.shape
    FF = wg.shape[2]
    H = D // 2
    SL = LO + HI
    CH = S * SL
    HT = T // 2
    PR = 2 * SL
    LAST = EPD + 1
    NG, NDT = FF // CT, D // CT
    HTILES = H // CT
    me = lax.axis_index("ep")
    px, py = lax.div(me, S), lax.rem(me, S)

    def dev(p, df, ds):
        dx = df * (1 - p) + ds * p
        dy = df * p + ds * (1 - p)
        return lax.rem(px + dx, S) * S + lax.rem(py + dy, S)

    def lo(r):
        return (r // 2) * PR + (r % 2) * LO

    def hi(r):
        return (r // 2) * PR + 2 * LO + (r % 2) * HI

    def start_gu(n):
        slot = lax.rem(n, GB)
        u, c = lax.div(n, NG), lax.rem(n, NG)

        @pl.when(jnp.logical_or(u == 0, u == LAST))
        def _():
            at = cols(c + lax.div(u, LAST) * NG)
            pltpu.make_async_copy(sg.at[:, at], gu.at[slot, 0], gu_sem.at[slot, 0]).start()
            pltpu.make_async_copy(su.at[:, at], gu.at[slot, 1], gu_sem.at[slot, 1]).start()

        @pl.when(jnp.logical_and(u > 0, u < LAST))
        def _():
            pltpu.make_async_copy(wg.at[u - 1, :, cols(c)], gu.at[slot, 0], gu_sem.at[slot, 0]).start()
            pltpu.make_async_copy(wu.at[u - 1, :, cols(c)], gu.at[slot, 1], gu_sem.at[slot, 1]).start()

    def wait_gu(n):
        slot = lax.rem(n, GB)
        for j in range(2):
            pltpu.make_async_copy(sg.at[:, cols(0)], gu.at[slot, j], gu_sem.at[slot, j]).wait()
        return slot

    def start_db(m):
        slot = lax.rem(m, DB)
        u, c = lax.div(m, NDT), lax.rem(m, NDT)

        @pl.when(jnp.logical_or(u == 0, u == LAST))
        def _():
            rows = pl.ds(pl.multiple_of(lax.div(u, LAST) * FF, FF), FF)
            pltpu.make_async_copy(sd.at[rows, cols(c)], db.at[slot], db_sem.at[slot]).start()

        @pl.when(jnp.logical_and(u > 0, u < LAST))
        def _():
            pltpu.make_async_copy(wd.at[u - 1, :, cols(c)], db.at[slot], db_sem.at[slot]).start()

    def wait_db(m):
        slot = lax.rem(m, DB)
        pltpu.make_async_copy(wd.at[0, :, cols(0)], db.at[slot], db_sem.at[slot]).wait()
        return slot

    x_copy = pltpu.make_async_copy(x_hbm, x_ref, x_sem)
    routing = [
        pltpu.make_async_copy(a, b, i_sem.at[i])
        for i, (a, b) in enumerate(
            ((expert_hbm, expert_ref), (slot_hbm, slot_ref), (gate_hbm, gate_ref))
        )
    ]
    barrier = pltpu.get_barrier_semaphore()
    for p in range(2):
        for d in range(1, S):
            pl.semaphore_signal(barrier, inc=1, device_id={"ep": dev(p, d, 0)})
    for copy in routing:
        copy.start()
    x_copy.start()
    for n in range(GB - 1):
        start_gu(jnp.int32(n))
    for m in range(DB - 1):
        start_db(jnp.int32(m))
    pl.semaphore_wait(barrier, 2 * (S - 1))

    def remote(src, dst, s, r, to):
        return pltpu.make_async_remote_copy(src, dst, s, r, device_id={"ep": to})

    def ag_first(p, d, early):
        i = 0 if d == 1 else 1
        rows = pl.ds((i if early else 1 - i) * HT, HT)
        n = i if early else 2 + i
        return remote(
            x_hbm.at[rows, pl.ds(p * H, H)], ag.at[p, S - d - 1, rows],
            ag_s.at[p, n], ag_r.at[p, n], dev(p, d, 0),
        )

    def ag_relay(p, d):
        i = 0 if d == 1 else 1
        rows = pl.ds(i * HT, HT)
        src = ag.at[p, (S - 1 if d == 1 else 1) - 1, rows]
        return remote(src, ag.at[p, 1, rows], ag_s.at[p, 4 + i], ag_r.at[p, 4 + i], dev(p, d, 0))

    def meta_copy(p, d):
        return remote(meta_ref, mall.at[p, S - d], m_s.at[p, d - 1], m_r.at[p, S - d - 1], dev(p, d, 0))

    for early in (True, False):
        for p in range(2):
            for d in (1, S - 1):
                ag_first(p, d, early).start()

    for copy in routing:
        copy.wait()
    meta_ref[...] = jnp.zeros(meta_ref.shape, F32)
    for j in range(TOP):
        slot = slot_ref[j]
        meta_ref[j : j + 1] = jnp.where(slot < SL, expert_ref[j] * SL + slot, -1).astype(F32)
        meta_ref[8 + j : 9 + j] = gate_ref[j]
    for p in range(2):
        mall[p, 0] = meta_ref[...]
        for d in range(1, S):
            meta_copy(p, d).start()

    def up(lhs, rows, u):
        def tile(i, _):
            n = u * NG + i
            slot = wait_gu(n)
            pl.when(n + GB - 1 < (LAST + 1) * NG)(lambda: start_gu(n + GB - 1))
            g = dot(lhs[...], gu[slot, 0])
            v = dot(lhs[...], gu[slot, 1])
            h[0:rows, cols(i)] = (jax.nn.silu(g) * v).astype(BF16)
            return 0

        lax.fori_loop(0, NG, tile, 0)

    def down_tile(rows, u, c):
        m = u * NDT + c
        slot = wait_db(m)
        pl.when(m + DB - 1 < (LAST + 1) * NDT)(lambda: start_db(m + DB - 1))
        return dot(h[0:rows, :], db[slot])

    def shared_down(u):
        def tile(c, _):
            o = down_tile(T, u, c)
            ysh[:, cols(c)] = o if u == 0 else ysh[:, cols(c)] + o
            return 0

        lax.fori_loop(0, NDT, tile, 0)

    x_copy.wait()
    up(x_ref, T, 0)
    for p in range(2):
        for d in (1, S - 1):
            ag_first(p, d, True).wait_recv()
        ag_relay(p, 1).start()
        ag_relay(p, S - 1).start()
    shared_down(0)

    for p in range(2):
        for d in (1, S - 1):
            ag_first(p, d, False).wait_recv()
        for d in range(1, S):
            meta_copy(p, d).wait_recv()

    def source(p, r, c):
        if r == 0:
            return x_ref[:, pl.ds(pl.multiple_of(p * H + c * CT, CT), CT)]
        return ag[p, r - 1, :, cols(c)]

    def onehot(p, r):
        i = lax.broadcasted_iota(jnp.int32, (S * EPD * SL, T), 0)
        n = EPD * SL
        off = dev(p, 0, S - 1) * n - (S - 1) * n
        for k in range(S - 2, -1, -1):
            off = jnp.where(i < (k + 1) * n, (dev(p, 0, k) - k) * n, off)
        code = (i + off).astype(F32)
        total = jnp.zeros(code.shape, F32)
        for j in range(TOP):
            total += jnp.where(code == mall[p, r, j : j + 1, :], 1.0, 0.0)
        return total.astype(BF16)

    def select(p, pair):
        for j in range(2):
            oh[j] = onehot(p, 2 * pair + j)

        def tile(c, _):
            a = dot(oh[0], source(p, 2 * pair, c))
            b = dot(oh[1], source(p, 2 * pair + 1, c))
            for k in range(S):
                for e in range(EPD):
                    o = (k * EPD + e) * SL
                    m = o + LO
                    b48 = jnp.concatenate([a[o:m], b[o:m], a[m : o + SL], b[m : o + SL]], 0)
                    at = pair * PR
                    if k == 0:
                        z[p, e, 0, at : at + PR, cols(c)] = b48.astype(BF16)
                    else:
                        at += e * CH
                        dsend[p, k - 1, at : at + PR, cols(c)] = b48.astype(BF16)
            return 0

        lax.fori_loop(0, HTILES, tile, 0)

    def halves(e):
        return (0, 1) if e < EARLY else (2,)

    def z_copy(p, e, k, half):
        at, n = (half * PR, PR) if half < 2 else (0, CH)
        rows = pl.ds(pl.multiple_of(e * CH + at, PR), n)
        return remote(
            dsend.at[p, k - 1, rows], z.at[p, e, S - k, pl.ds(at, n)],
            z_s.at[p, e, k - 1, half % 2], z_r.at[p, e, S - k - 1, half % 2], dev(p, 0, k),
        )

    def z_start(e, half):
        for k in (1, S - 1, 2):
            for p in range(2):
                z_copy(p, e, k, half).start()

    for p in range(2):
        select(p, 0)
    for e in range(EARLY):
        z_start(e, 0)
    for p in range(2):
        for d in (1, S - 1):
            ag_relay(p, d).wait_recv()
    for p in range(2):
        select(p, 1)
    for e in range(EPD):
        z_start(e, 1 if e < EARLY else 2)

    def coefficients(n, _):
        p, r = lax.div(n, S), lax.rem(n, S)
        half = EPD * S * LO
        i = lax.broadcasted_iota(jnp.int32, (2 * half, T), 0)
        high = i >= half
        i = jnp.where(high, i - half, i)
        e, kk, c = i >> 6, (i >> 4) & 3, i & 15
        owner = jnp.where(kk == 0, dev(p, 0, 0), 0)
        for k in range(1, S):
            owner = jnp.where(kk == k, dev(p, 0, k), owner)
        odd = c >> 3
        slot = jnp.where(high, LO + (c & 7), c)
        code = (owner * EPD + e) * SL + slot
        code = jnp.where(jnp.logical_and(high, odd != lax.rem(r, 2)), -2, code).astype(F32)
        total = jnp.zeros(code.shape, F32)
        for j in range(TOP):
            total += jnp.where(code == mall[p, r, j : j + 1, :], mall[p, r, 8 + j : 9 + j, :], 0.0)
        cmat[p, r] = total.T.astype(BF16)
        return 0

    lax.fori_loop(0, 2 * S, coefficients, 0)

    def c_copy(p, e, k, half):
        at, n = (half * PR, PR) if half < 2 else (0, CH)
        return remote(
            z.at[p, e, k, pl.ds(at, n)], crecv.at[p, e, S - k, pl.ds(at, n)],
            c_s.at[p, e, k - 1, half % 2], c_r.at[p, e, S - k - 1, half % 2], dev(p, 0, k),
        )

    def expert(e, _):
        def arrived(half):
            for k in (1, S - 1, 2):
                for p in range(2):
                    z_copy(p, e, k, half).wait_recv()

        @pl.when(e < EARLY)
        def _():
            arrived(0)
            arrived(1)

        @pl.when(e >= EARLY)
        def _():
            arrived(2)

        for k in range(S):
            zf[k * CH : (k + 1) * CH, 0:H] = z[0, e, k]
            for r in range(S):
                o = k * CH + lo(r)
                zf[o : o + LO, H:D] = z[1, e, r, lo(k) : lo(k) + LO]
            u0 = hi(k) - (k % 2) * HI
            for r in range(0, S, 2):
                o = k * CH + hi(r)
                two = [
                    z[1, e, r + j, u0 : u0 + 2 * HI].astype(F32)[(k % 2) * HI : (k % 2 + 1) * HI]
                    for j in range(2)
                ]
                zf[o : o + 2 * HI, H:D] = jnp.concatenate(two, 0).astype(BF16)

        up(zf, S * CH, 1 + e)

        def back(p, half):
            for k in (1, S - 1, 2):
                c_copy(p, e, k, half).start()

        for p in range(2):

            def tile(c, _):
                o = down_tile(S * CH, 1 + e, p * HTILES + c)
                for k in range(S):
                    if p == 0:
                        b = o[k * CH : (k + 1) * CH]
                    else:
                        rows = []
                        for r in range(0, S, 2):
                            for f, n in ((lo(k), LO), (hi(k), HI)):
                                rows += [o[q * CH + f : q * CH + f + n] for q in (r, r + 1)]
                        b = jnp.concatenate(rows, 0)
                    if k == 0:
                        crecv[p, e, 0, :, cols(c)] = b.astype(BF16)
                    else:
                        z[p, e, k, :, cols(c)] = b.astype(BF16)
                return 0

            lax.fori_loop(0, HTILES, tile, 0)
            pl.when(e < EPD - 1)(lambda: back(p, 2))

        @pl.when(e == EPD - 1)
        def _():
            for half in (1, 0):
                for p in range(2):
                    back(p, half)

        return 0

    lax.fori_loop(0, EPD, expert, 0)
    up(x_ref, T, LAST)
    shared_down(LAST)

    for p in range(2):
        for e in range(EPD):
            for k in range(1, S):
                for half in halves(e):
                    z_copy(p, e, k, half).wait_send()

    def slots(p, r, c):
        a = crecv[p, :, :, lo(r) : lo(r) + LO, cols(c)].reshape(EPD * S * LO, CT)
        u0 = hi(r) - (r % 2) * HI
        b = crecv[p, :, :, u0 : u0 + 2 * HI, cols(c)].reshape(EPD * S * LO, CT)
        return jnp.concatenate([a, b], 0)

    def part(p, r, c, r0, r1):
        return dot(cmat[p, r, r0:r1], slots(p, r, c))

    def via_copy(p, i):
        src = dsend.at[p, 1, pl.ds(i * HT, HT)]
        return remote(src, via.at[p, i], v_s.at[p, i], v_r.at[p, i], dev(p, 1 if i == 0 else S - 1, 0))

    def fin_copy(p, i, half):
        src = dsend.at[p, 2 * i, pl.ds(half * HT, HT)]
        if half == i:
            dst = late_ref.at[pl.ds(half * HT, HT), pl.ds(p * H, H)]
        else:
            dst = fin.at[p, i]
        return remote(src, dst, f_s.at[p, i, half], f_r.at[p, i, half], dev(p, 1 if i == 0 else S - 1, 0))

    for p in range(2):
        for e in range(EPD):
            for k in range(1, S):
                c_copy(p, e, k, 2 if e < EPD - 1 else 1).wait_recv()

        def far(c, _):
            dsend[p, 1, 0:T, cols(c)] = part(p, 2, c, 0, T).astype(BF16)
            return 0

        lax.fori_loop(0, HTILES, far, 0)
        for i in range(2):
            via_copy(p, i).start()

    for p in range(2):

        def before(c, _):
            dsend[p, 2, 0:HT, cols(c)] = part(p, S - 1, c, 0, HT).astype(BF16)
            return 0

        lax.fori_loop(0, HTILES, before, 0)
        fin_copy(p, 1, 0).start()

    for p in range(2):
        for k in range(1, S):
            c_copy(p, EPD - 1, k, 0).wait_recv()

        def after(c, _):
            dsend[p, 0, HT:T, cols(c)] = part(p, 1, c, HT, T).astype(BF16)
            return 0

        lax.fori_loop(0, HTILES, after, 0)
        fin_copy(p, 0, 1).start()

    for p in range(2):
        for i in range(2):
            via_copy(p, i).wait_recv()

        def through(c, _):
            a = part(p, 1, c, 0, HT) + via[p, 0, :, cols(c)].astype(F32)
            b = part(p, S - 1, c, HT, T) + via[p, 1, :, cols(c)].astype(F32)
            dsend[p, 0, 0:HT, cols(c)] = a.astype(BF16)
            dsend[p, 2, HT:T, cols(c)] = b.astype(BF16)
            return 0

        lax.fori_loop(0, HTILES, through, 0)
        fin_copy(p, 0, 0).start()
        fin_copy(p, 1, 1).start()

    for p in range(2):

        def own(c, _):
            ysh[:, cols(p * HTILES + c)] += part(p, 0, c, 0, T)
            return 0

        lax.fori_loop(0, HTILES, own, 0)

    def y_copy(p):
        half = pl.ds(p * H, H)
        return pltpu.make_async_copy(ysh.at[:, half], sum_ref.at[:, half], y_sem.at[p])

    for p in range(2):
        for i in range(2):
            fin_copy(p, i, 1 - i).wait_recv()

        def last(c, _):
            at = cols(p * HTILES + c)
            ysh[0:HT, at] += fin[p, 1, :, cols(c)].astype(F32)
            ysh[HT:T, at] += fin[p, 0, :, cols(c)].astype(F32)
            return 0

        lax.fori_loop(0, HTILES, last, 0)
        y_copy(p).start()
    for p in range(2):
        y_copy(p).wait()
        for i in range(2):
            fin_copy(p, i, i).wait_recv()

    for p in range(2):
        for d in range(1, S):
            meta_copy(p, d).wait_send()
        for d in (1, S - 1):
            for early in (True, False):
                ag_first(p, d, early).wait_send()
            ag_relay(p, d).wait_send()
        for e in range(EPD):
            for k in range(1, S):
                for half in (2,) if e < EPD - 1 else (0, 1):
                    c_copy(p, e, k, half).wait_send()
        for i in range(2):
            via_copy(p, i).wait_send()
            for half in range(2):
                fin_copy(p, i, half).wait_send()


def add(a_ref, b_ref, y_ref):
    y_ref[...] = (a_ref[...] + b_ref[...].astype(F32)).astype(y_ref.dtype)


def solution(mesh):
    side = math.isqrt(mesh.shape["ep"])

    def local(x, expert, slot, gate, w_gate, w_up, w_down, s_gate, s_up, s_down):
        T, D = x.shape[2:]
        TOP = expert.shape[3]
        EPD, _, FF = w_gate.shape
        SL, S, H = LO + HI, side, D // 2
        assert side * side == mesh.shape["ep"] and side == 4
        assert FF * 2 == s_gate.shape[1] and SL == 5 * T * TOP // (4 * EPD * mesh.shape["ep"])
        rows = EPD * S * SL
        sem = pltpu.SemaphoreType.DMA
        total, late = pl.pallas_call(
            functools.partial(kernel, S, EPD, TOP),
            out_shape=[jax.ShapeDtypeStruct((T, D), F32), jax.ShapeDtypeStruct((T, D), BF16)],
            in_specs=[pl.BlockSpec(memory_space=pl.ANY)] * 10,
            out_specs=[pl.BlockSpec(memory_space=pl.ANY)] * 2,
            scratch_shapes=[
                pltpu.VMEM((T, D), BF16),
                pltpu.VMEM((TOP, 1, T), jnp.int32),
                pltpu.VMEM((TOP, 1, T), jnp.int32),
                pltpu.VMEM((TOP, 1, T), F32),
                pltpu.VMEM((16, T), F32),
                pltpu.VMEM((2, S - 1, T, H), BF16),
                pltpu.VMEM((2, S, 16, T), F32),
                pltpu.VMEM((2, rows, T), BF16),
                pltpu.VMEM((2, S - 1, rows, H), BF16),
                pltpu.VMEM((2, EPD, S, S * SL, H), BF16),
                pltpu.VMEM((S * S * SL, D), BF16),
                pltpu.VMEM((2, EPD, S, S * SL, H), BF16),
                pltpu.VMEM((2, 2, T // 2, H), BF16),
                pltpu.VMEM((2, 2, T // 2, H), BF16),
                pltpu.VMEM((2, S, T, 2 * EPD * S * LO), BF16),
                pltpu.VMEM((S * S * SL, FF), BF16),
                pltpu.VMEM((T, D), F32),
                pltpu.VMEM((GB, 2, D, CT), BF16),
                pltpu.VMEM((DB, FF, CT), BF16),
                sem, sem((3,)), sem((2,)), sem((GB, 2)), sem((DB,)),
                sem((2, 6)), sem((2, 6)),
                sem((2, S - 1)), sem((2, S - 1)),
                sem((2, EPD, S - 1, 2)), sem((2, EPD, S - 1, 2)),
                sem((2, EPD, S - 1, 2)), sem((2, EPD, S - 1, 2)),
                sem((2, 2)), sem((2, 2)),
                sem((2, 2, 2)), sem((2, 2, 2)),
            ],
            compiler_params=pltpu.CompilerParams(
                collective_id=0, has_side_effects=True, vmem_limit_bytes=67043328
            ),
        )(x.reshape(T, D), *(v.transpose(0, 3, 1, 2).reshape(TOP, 1, T) for v in (expert, slot, gate)), w_gate, w_up, w_down, s_gate, s_up, s_down)
        y = pl.pallas_call(
            add,
            grid=(PARTS,),
            out_shape=jax.ShapeDtypeStruct((T, D), x.dtype),
            in_specs=[pl.BlockSpec((T // PARTS, D), lambda i: (i, 0))] * 2,
            out_specs=pl.BlockSpec((T // PARTS, D), lambda i: (i, 0)),
        )(total, late)
        return y.reshape(x.shape)

    own, experts, whole = P("dp", "ep"), P("ep"), P()
    return jax.shard_map(
        local,
        mesh=mesh,
        in_specs=(own,) * 4 + (experts,) * 3 + (whole,) * 3,
        out_specs=own,
        check_vma=False,
    )
```
